32 devices in a mesh: dp: 4 (over x, y), tp: 8 (over z, core).
Axes of the slice: x: 2, y: 2, z: 4, core: 2. Of those that a mesh axis runs over, the one named last changes fastest.
Arguments:
- x: bfloat16 [8192, 7168], P(('dp', 'tp')), parts along dimension 0
- gain: bfloat16 [7168], replicated
- wq: bfloat16 [7168, 7168], P(None, 'tp')
- wk: bfloat16 [7168, 7168], P(None, 'tp')
- wv: bfloat16 [7168, 7168], P(None, 'tp')
- wo: bfloat16 [7168, 7168], P('tp')
Outputs:
- output: bfloat16 [8192, 7168], P(('dp', 'tp')), parts along dimension 0
There are 4 independent parts. The reference program is written for one: setup_inputs(seed, part) draws one part's arguments, and reference() takes and returns one part's arrays. A program takes and returns all parts, laid end to end along the dimension named above; an argument that names none is the same for every part.
All inputs are finite; a program needn't handle non-finite values.
Results may differ from the reference program's by a relative error of at most 0.012.
Values are sent between devices in bfloat16 or wider.
A program may use at most 2 GiB of HBM per device.

```python
import jax
import jax.numpy as jnp
from jax import lax

ROWS = 2048
D = 7168
HEADS = 56
KV_HEADS = 56
HEAD = 128
THETA = 10000


def setup_inputs(seed: int = 0, part: int = 0) -> dict:
    kx, kn, kq, kk, kv, ko = jax.random.split(jax.random.key(seed), 6)

    def weights(key, rows, columns):
        return jax.random.normal(key, (rows, columns), jnp.float32) * rows**-0.5

    drawn = {
        "x": jax.random.normal(jax.random.fold_in(kx, part), (ROWS, D), jnp.float32),
        "gain": 1 + 0.1 * jax.random.normal(kn, (D,), jnp.float32),
        "wq": 2 * weights(kq, D, HEADS * HEAD),
        "wk": 2 * weights(kk, D, KV_HEADS * HEAD),
        "wv": 4 * weights(kv, D, KV_HEADS * HEAD),
        "wo": weights(ko, HEADS * HEAD, D),
    }
    return {k: v.astype(jnp.bfloat16) for k, v in drawn.items()}


def normed(x, gain):
    wide = x.astype(jnp.float32)
    scale = lax.rsqrt(jnp.mean(wide * wide, -1, keepdims=True) + 1e-6)
    return (wide * scale * gain.astype(jnp.float32)).astype(jnp.bfloat16)


def turned(t, place, theta):
    half = t.shape[-1] // 2
    angle = place.astype(jnp.float32)[:, None] * theta ** (-jnp.arange(half, dtype=jnp.float32) / half)
    cos, sin = jnp.cos(angle)[:, None], jnp.sin(angle)[:, None]
    a, b = t[..., :half].astype(jnp.float32), t[..., half:].astype(jnp.float32)
    return jnp.concatenate([a * cos - b * sin, b * cos + a * sin], -1).astype(jnp.bfloat16)


def matmul(a, w):
    return jnp.dot(a, w, preferred_element_type=jnp.float32).astype(jnp.bfloat16)


def einsum(form, a, b):
    return jnp.einsum(form, a.astype(jnp.float32), b.astype(jnp.float32))


def attention(q, k, v):
    scores = einsum("tgsd,ugd->gstu", q, k) * q.shape[-1] ** -0.5
    token = jnp.arange(q.shape[0])
    scores = jnp.where(token[:, None] >= token, scores, -jnp.inf)
    weights = jax.nn.softmax(scores, -1).astype(jnp.bfloat16)
    return einsum("gstu,ugd->tgsd", weights, v).astype(jnp.bfloat16)


def reference(x, gain, wq, wk, wv, wo):
    a, place = normed(x, gain), jnp.arange(ROWS)
    q = turned(matmul(a, wq).reshape(ROWS, HEADS, HEAD), place, THETA).reshape(ROWS, KV_HEADS, -1, HEAD)
    k = turned(matmul(a, wk).reshape(ROWS, KV_HEADS, HEAD), place, THETA)
    v = matmul(a, wv).reshape(ROWS, KV_HEADS, HEAD)
    seen = attention(q, k, v).reshape(ROWS, HEADS * HEAD)
    return (x.astype(jnp.float32) + jnp.dot(seen, wo, preferred_element_type=jnp.float32)).astype(jnp.bfloat16)
```

```python
import functools

import jax
import jax.numpy as jnp
from jax import lax
from jax.experimental import pallas as pl
from jax.experimental.pallas import tpu as pltpu
from jax.sharding import PartitionSpec as P

HEAD = 128
THETA = 10000
NEG = -1e30
HIDDEN = 2 * NEG
LOG2E = 1.4426950408889634
CHIPS = 4
BLOCKS = 8
UNITS = 4
MESH = pl.DeviceIdType.MESH


def _dot(a, b, ca, cb):
    return lax.dot_general(a, b, (((ca,), (cb,)), ((), ())), preferred_element_type=jnp.float32)


def _need(c, b):
    n0 = jnp.maximum(4 * (b - 1), 0)
    n1 = jnp.where(b < 2, 4 * (b + 1), jnp.where(b == 2, 10, jnp.where(b == 3, 13, 16)))
    n2 = jnp.minimum(4 * (b + 1), 16)
    n3 = jnp.minimum(4 * (b + 1), 24)
    return jnp.where(c == 0, n0, jnp.where(c == 1, n1, jnp.where(c == 2, n2, n3)))


def _slots(c):
    return 8 * jnp.maximum(c, CHIPS - 1 - c)


def _order(c, r):
    o1 = jnp.where(r < 4, r // 2 + 4 * (r % 2), 6 - 4 * (r % 2) + (r - 4) // 2)
    o2 = jnp.where(r == 5, 6, jnp.where(r == 6, 5, r))
    return jnp.where(c == 0, (r + 2) % 8, jnp.where(c == 1, o1, jnp.where(c == 2, o2, r)))


def _summed(c, b):
    s0 = jnp.maximum(b - 1, 0)
    s1 = jnp.maximum(2 * (b - 4), 0)
    s2 = jnp.where(b == 6, 4, jnp.maximum(b - 1, 0))
    s3 = jnp.minimum(b + 1, 6)
    s = jnp.where(c == 0, s0, jnp.where(c == 1, s1, jnp.where(c == 2, s2, s3)))
    return jnp.where(b == 7, 8, s)


def layer(x_ref, gain_ref, turn_ref, wq_ref, wk_ref, wv_ref, wo_ref, own_out, fin_out, xg, own_s, sib_in, left_in, right_in,
          xv, gain_v, turn_v, wbuf, wobuf, acc, qv, kc, vt, ov, top_s, mix_s, tbuf, tst, rs_own, rs_sib, rs_l, rs_r, rs_out,
          lsem, wsem, osem, tsem, tssem, recv_r, recv_l, recv_o, recv_s, send_r, send_l, send_o, send_s,
          recv_t, recv_rl, recv_rr, recv_f, out_sem, fsem):
    t = lax.axis_index("tp")
    c, k = t // 2, t % 2
    me, sib, left, right = {"tp": t}, {"tp": t + 1 - 2 * k}, {"tp": t - 2}, {"tp": t + 2}
    mine, other = 2 * c + k, 2 * c + 1 - k
    heads, rows = qv.shape[0], qv.shape[1]
    depth, width = wbuf.shape[2], wbuf.shape[3]
    steps = xv.shape[2] // depth
    wide = wobuf.shape[2]
    first, final = c == 0, c == CHIPS - 1

    def remote(src, dst, ssem, rsem, to):
        return pltpu.make_async_remote_copy(src_ref=src, dst_ref=dst, send_sem=ssem, recv_sem=rsem, device_id=to, device_id_type=MESH)

    def unit(b, h, j):
        return xg.at[(b * 2 + h) * UNITS + j]

    def to_right(b, j):
        u = unit(b, k, j)
        return remote(u, u, send_r.at[b * UNITS + j], recv_r.at[b * UNITS + j], right)

    def to_left(b, j):
        u = unit(b, k, j)
        return remote(u, u, send_l.at[b * UNITS + j], recv_l.at[b * UNITS + j], left)

    def to_sib(b, j):
        u = unit(b, k, j)
        return remote(u, u, send_s.at[b * UNITS + j], recv_s.at[b * UNITS + j], sib)

    def own_to_sib(h, j):
        u = unit(mine, h, j)
        return remote(u, u, send_o.at[h * UNITS + j], recv_o.at[h * UNITS + j], sib)

    def fetch_w(g):
        at, slot = pl.multiple_of((g % steps) * depth, depth), g % 2
        return [pltpu.make_async_copy(w.at[pl.ds(at, depth), :], wbuf.at[slot, i], wsem.at[slot, i])
                for i, w in enumerate((wq_ref, wk_ref, wv_ref))]

    def fetch_wo(j):
        return pltpu.make_async_copy(wo_ref.at[:, pl.ds(pl.multiple_of(j * wide, 128), wide)], wobuf.at[j % 2], osem.at[j % 2])

    barrier = pltpu.get_barrier_semaphore()
    pl.semaphore_signal(barrier, inc=1, device_id=sib, device_id_type=MESH)

    @pl.when(jnp.logical_not(first))
    def _():
        pl.semaphore_signal(barrier, inc=1, device_id=left, device_id_type=MESH)

    @pl.when(jnp.logical_not(final))
    def _():
        pl.semaphore_signal(barrier, inc=1, device_id=right, device_id_type=MESH)

    load_x = pltpu.make_async_copy(x_ref, xv, lsem.at[0])
    load_g = pltpu.make_async_copy(gain_ref, gain_v, lsem.at[1])
    load_x.start()
    load_g.start()
    for cp in fetch_w(0):
        cp.start()
    load_x.wait()
    load_g.wait()

    def norm(n, _):
        at = (n // 2, pl.ds(pl.multiple_of((n % 2) * (xv.shape[1] // 2), xv.shape[1] // 2), xv.shape[1] // 2))
        wx = xv[at[0], at[1], :].astype(jnp.float32)
        scale = lax.rsqrt(jnp.mean(wx * wx, -1, keepdims=True) + 1e-6)
        xv[at[0], at[1], :] = (wx * scale * gain_v[...].astype(jnp.float32)).astype(jnp.bfloat16)

    lax.fori_loop(0, 16, norm, None)
    keep = pltpu.make_async_copy(xv, xg.at[pl.ds(mine * 8, 8)], lsem.at[0])
    keep.start()
    keep.wait()

    middle = jnp.logical_and(jnp.logical_not(first), jnp.logical_not(final))

    @pl.when(middle)
    def _():
        pl.semaphore_wait(barrier, 3)

    @pl.when(jnp.logical_not(middle))
    def _():
        pl.semaphore_wait(barrier, 2)

    for n in range(8):
        h = 1 - k if n < 4 else k
        own_to_sib(h, n % 4).start()

    def begin(i, _):
        b, j = 2 * c + i // UNITS, i % UNITS

        @pl.when(b == other)
        def _():
            u = unit(other, k, j)
            remote(u, u, send_o.at[k * UNITS + j], recv_o.at[k * UNITS + j], sib).wait_recv()

        @pl.when(jnp.logical_not(first))
        def _():
            to_left(b, j).start()

        @pl.when(first)
        def _():
            to_right(b, j).start()

    lax.fori_loop(0, 2 * UNITS, begin, None)
    for h in range(heads):
        vt[h, HEAD:, :] = jnp.ones((vt.shape[1] - HEAD, vt.shape[2]), jnp.bfloat16)

    def slot(i, _):
        j = i % UNITS

        @pl.when(i < 8 * c)
        def _():
            b = i // UNITS
            to_right(b, j).wait_recv()

            @pl.when(jnp.logical_not(final))
            def _():
                to_right(b, j).start()

            to_sib(b, j).start()

            @pl.when(jnp.logical_and(jnp.logical_not(final), i == 8 * c - 1))
            def _():
                def own(n, _):
                    to_right(2 * c + n // UNITS, n % UNITS).start()

                lax.fori_loop(0, 2 * UNITS, own, None)

        @pl.when(i < 8 * (CHIPS - 1 - c))
        def _():
            b = 2 * c + 2 + i // UNITS
            to_left(b, j).wait_recv()

            @pl.when(jnp.logical_not(first))
            def _():
                to_left(b, j).start()

            to_sib(b, j).start()

    def attend(b):
        e = HEAD**-0.5 * LOG2E
        top_s[...] = jnp.full(top_s.shape, NEG, jnp.float32)
        mix_s[...] = jnp.zeros(mix_s.shape, jnp.float32)

        def block(j, masked):
            here = pl.ds(pl.multiple_of(j * rows, rows), rows)
            scores = [_dot(kc[h, here, :], qv[h], 1, 1) for h in range(heads)]
            weights, keeps = [], []
            for h, s in enumerate(scores):
                if masked:
                    ok = lax.broadcasted_iota(jnp.int32, s.shape, 1) >= lax.broadcasted_iota(jnp.int32, s.shape, 0)
                    s = jnp.where(ok, s, HIDDEN)
                old = top_s[h : h + 1, :]
                top = jnp.maximum(old, s.max(axis=0, keepdims=True))
                top_s[h : h + 1, :] = top
                weights.append(jnp.exp2((s - top) * e).astype(jnp.bfloat16))
                keeps.append(jnp.exp2((old - top) * e))
            for h in range(heads):
                mix_s[h] = mix_s[h] * keeps[h] + _dot(vt[h, :, here], weights[h], 1, 0)

        lax.fori_loop(0, b, lambda j, _: block(j, False), None)
        block(b, True)
        for h in range(heads):
            total = mix_s[h, HEAD : HEAD + 1, :]
            ov[:, h * HEAD : (h + 1) * HEAD] = (mix_s[h, :HEAD, :] * (1 / total)).T.astype(jnp.bfloat16)

    def total_of(r, _):
        b = _order(c, r)
        d = b // 2
        own = pltpu.make_async_copy(own_s.at[b], rs_own, lsem.at[0])
        own.start()
        remote(sib_in.at[b], sib_in.at[b], tssem.at[0], recv_t.at[b], sib).wait_recv()
        theirs = pltpu.make_async_copy(sib_in.at[b], rs_sib, lsem.at[1])
        theirs.start()
        own.wait()
        theirs.wait()
        from_left = jnp.logical_and(d >= c, jnp.logical_not(first))
        from_right = jnp.logical_and(d <= c, jnp.logical_not(final))

        def part(j, _):
            place = (r * UNITS + j) % rs_out.shape[0]
            cols = pl.ds(pl.multiple_of(j * wide, 128), wide)
            get_l = pltpu.make_async_copy(left_in.at[b, j], rs_l, lsem.at[2])
            get_r = pltpu.make_async_copy(right_in.at[b, j], rs_r, lsem.at[3])

            @pl.when(from_left)
            def _():
                remote(rs_out.at[place], left_in.at[b, j], out_sem.at[place], recv_rl.at[b * UNITS + j], left).wait_recv()
                get_l.start()

            @pl.when(from_right)
            def _():
                remote(rs_out.at[place], right_in.at[b, j], out_sem.at[place], recv_rr.at[b * UNITS + j], right).wait_recv()
                get_r.start()

            rs_own[j] = rs_own[j] + rs_sib[j].astype(jnp.float32)

            @pl.when(from_left)
            def _():
                get_l.wait()
                rs_own[j] = rs_own[j] + rs_l[...].astype(jnp.float32)

            @pl.when(from_right)
            def _():
                get_r.wait()
                rs_own[j] = rs_own[j] + rs_r[...].astype(jnp.float32)

            @pl.when(b == mine)
            def _():
                pltpu.make_async_copy(rs_own.at[j], own_out.at[:, cols], fsem.at[j]).start()

            @pl.when(jnp.logical_and(r >= 2, _order(c, r - 2) != mine))
            def _():
                remote(rs_out.at[place], left_in.at[b, j], out_sem.at[place], recv_rl.at[b * UNITS + j], left).wait_send()

            @pl.when(b != mine)
            def _():
                rs_out[place] = rs_own[j].astype(jnp.bfloat16)

            @pl.when(d > c)
            def _():
                remote(rs_out.at[place], left_in.at[b, j], out_sem.at[place], recv_rl.at[b * UNITS + j], right).start()

            @pl.when(d < c)
            def _():
                remote(rs_out.at[place], right_in.at[b, j], out_sem.at[place], recv_rr.at[b * UNITS + j], left).start()

            @pl.when(b == other)
            def _():
                remote(rs_out.at[place], fin_out.at[:, cols], out_sem.at[place], recv_f.at[j], sib).start()

        lax.fori_loop(0, UNITS, part, None)

        @pl.when(b == mine)
        def _():
            for j in range(UNITS):
                pltpu.make_async_copy(rs_own.at[j], own_out.at[:, pl.ds(j * wide, wide)], fsem.at[j]).wait()

    def work(b, _):
        done = jnp.where(b == 0, 0, jnp.minimum(_need(c, b - 1) + 2, _slots(c)))
        now = jnp.maximum(_need(c, b), done)
        lax.fori_loop(done, now, slot, None)
        some = jnp.minimum(now + 1, jnp.minimum(_need(c, b) + 2, _slots(c)))
        some = jnp.maximum(some, now)
        most = jnp.maximum(now, jnp.minimum(_need(c, b) + 2, _slots(c)))

        @pl.when(b // 2 != c)
        def _():
            for j in range(UNITS):
                u = unit(b, 1 - k, j)
                remote(u, u, send_s.at[b * UNITS + j], recv_s.at[b * UNITS + j], sib).wait_recv()

        @pl.when(b == other)
        def _():
            for j in range(UNITS):
                u = unit(b, 1 - k, j)
                remote(u, u, send_o.at[j], recv_o.at[(1 - k) * UNITS + j], sib).wait_recv()

        tokens = pltpu.make_async_copy(xg.at[pl.ds(b * 8, 8)], xv, lsem.at[0])
        turns = pltpu.make_async_copy(turn_ref.at[:, b], turn_v, lsem.at[1])
        tokens.start()
        turns.start()
        acc[...] = jnp.zeros(acc.shape, jnp.float32)
        for j in range(2):
            fetch_wo(j).start()
        tokens.wait()
        turns.wait()

        def project(s, _):
            g = b * steps + s

            @pl.when(g + 1 < BLOCKS * steps)
            def _():
                for cp in fetch_w(g + 1):
                    cp.start()

            for cp in fetch_w(g):
                cp.wait()
            a = xv[:, :, pl.ds(pl.multiple_of(s * depth, 128), depth)].reshape(rows, depth)
            for i in range(3):
                acc[i] = acc[i] + jnp.dot(a, wbuf[g % 2, i], preferred_element_type=jnp.float32)

        lax.fori_loop(0, steps, project, None)
        lax.fori_loop(now, some, slot, None)
        at = pl.ds(pl.multiple_of(b * rows, rows), rows)
        cos, sin = turn_v[0], turn_v[1]
        for h in range(heads):
            cols = slice(h * HEAD, (h + 1) * HEAD)
            q = acc[0, :, cols].astype(jnp.bfloat16).astype(jnp.float32)
            qv[h] = (q * cos + pltpu.roll(q, HEAD // 2, 1) * sin).astype(jnp.bfloat16)
            key = acc[1, :, cols].astype(jnp.bfloat16).astype(jnp.float32)
            kc[h, at, :] = (key * cos + pltpu.roll(key, HEAD // 2, 1) * sin).astype(jnp.bfloat16)
            vt[h, :HEAD, at] = acc[2, :, cols].T.astype(jnp.bfloat16)
        attend(b)
        lax.fori_loop(some, most, slot, None)

        def term(j, _):
            place = j % 2
            mine_out = pltpu.make_async_copy(tbuf.at[place, k], own_s.at[b, j], tsem.at[place])
            theirs_out = remote(tst.at[place], sib_in.at[b, j], tssem.at[place], recv_t.at[b], sib)

            @pl.when(j >= 2)
            def _():
                mine_out.wait()
                theirs_out.wait_send()

            fetch_wo(j).wait()
            tbuf[place] = jnp.dot(ov[...], wobuf[place], preferred_element_type=jnp.float32).reshape(tbuf.shape[1:])

            @pl.when(j + 2 < UNITS)
            def _():
                fetch_wo(j + 2).start()

            tst[place] = tbuf[place, 1 - k].astype(jnp.bfloat16)
            mine_out.start()
            theirs_out.start()

        lax.fori_loop(0, UNITS, term, None)
        for place in range(2):
            pltpu.make_async_copy(tbuf.at[place, k], own_s.at[b, place], tsem.at[place]).wait()
            remote(tst.at[place], sib_in.at[b, place], tssem.at[place], recv_t.at[b], sib).wait_send()
        lax.fori_loop(jnp.where(b == 0, 0, _summed(c, b - 1)), _summed(c, b), total_of, None)

    lax.fori_loop(0, BLOCKS, work, None)

    def sent(r, _):
        @pl.when(_order(c, r) != mine)
        def _():
            for j in range(UNITS):
                place = (r * UNITS + j) % rs_out.shape[0]
                remote(rs_out.at[place], left_in.at[0, j], out_sem.at[place], recv_rl.at[j], left).wait_send()

    lax.fori_loop(BLOCKS - 2, BLOCKS, sent, None)
    for j in range(UNITS):
        cols = pl.ds(j * wide, wide)
        remote(rs_out.at[0], fin_out.at[:, cols], out_sem.at[0], recv_f.at[j], sib).wait_recv()
    for n in range(8):
        own_to_sib(n // 4, n % 4).wait_send()

    def passed(i, _):
        b, j = i // UNITS, i % UNITS

        @pl.when(jnp.logical_and(jnp.logical_not(final), b <= 2 * c + 1))
        def _():
            to_right(b, j).wait_send()

        @pl.when(jnp.logical_and(jnp.logical_not(first), b >= 2 * c))
        def _():
            to_left(b, j).wait_send()

        @pl.when(b // 2 != c)
        def _():
            to_sib(b, j).wait_send()

    lax.fori_loop(0, BLOCKS * UNITS, passed, None)


def turns(rows):
    half = HEAD // 2
    angle = jnp.arange(rows).astype(jnp.float32)[:, None] * THETA ** (-jnp.arange(half, dtype=jnp.float32) / half)
    cos, sin = jnp.cos(angle), jnp.sin(angle)
    return jnp.stack([jnp.concatenate([cos, cos], -1), jnp.concatenate([-sin, sin], -1)])


def solution(mesh):
    def step(x, gain, wq, wk, wv, wo):
        rows, dim = x.shape
        width = wq.shape[1]
        heads, half, wide, depth = width // HEAD, rows // 2, dim // UNITS, dim // 7
        bf, f32 = jnp.bfloat16, jnp.float32
        hbm = pl.BlockSpec(memory_space=pl.ANY)
        dma = pltpu.SemaphoreType.DMA
        turn = turns(BLOCKS * rows).reshape(2, BLOCKS, rows, HEAD)
        shape = jax.ShapeDtypeStruct
        own, fin, *_ = pl.pallas_call(
            layer,
            out_shape=[
                shape((half, dim), f32),
                shape((half, dim), bf),
                shape((BLOCKS * 8, rows // 8, dim), bf),
                shape((BLOCKS, UNITS, half, wide), f32),
                shape((BLOCKS, UNITS, half, wide), bf),
                shape((BLOCKS, UNITS, half, wide), bf),
                shape((BLOCKS, UNITS, half, wide), bf),
            ],
            in_specs=[hbm] * 7,
            out_specs=[hbm] * 7,
            scratch_shapes=[
                pltpu.VMEM((8, rows // 8, dim), bf),
                pltpu.VMEM((1, dim), bf),
                pltpu.VMEM((2, rows, HEAD), f32),
                pltpu.VMEM((2, 3, depth, width), bf),
                pltpu.VMEM((2, width, wide), bf),
                pltpu.VMEM((3, rows, width), f32),
                pltpu.VMEM((heads, rows, HEAD), bf),
                pltpu.VMEM((heads, BLOCKS * rows, HEAD), bf),
                pltpu.VMEM((heads, HEAD + 16, BLOCKS * rows), bf),
                pltpu.VMEM((rows, width), bf),
                pltpu.VMEM((heads, rows), f32),
                pltpu.VMEM((heads, HEAD + 16, rows), f32),
                pltpu.VMEM((2, 2, half, wide), f32),
                pltpu.VMEM((2, half, wide), bf),
                pltpu.VMEM((UNITS, half, wide), f32),
                pltpu.VMEM((UNITS, half, wide), bf),
                pltpu.VMEM((half, wide), bf),
                pltpu.VMEM((half, wide), bf),
                pltpu.VMEM((8, half, wide), bf),
                dma((4,)), dma((2, 3)), dma((2,)), dma((2,)), dma((2,)),
                dma((24,)), dma((32,)), dma((8,)), dma((32,)),
                dma((32,)), dma((32,)), dma((8,)), dma((32,)),
                dma((8,)), dma((32,)), dma((32,)), dma((4,)), dma((8,)), dma((4,)),
            ],
            compiler_params=pltpu.CompilerParams(collective_id=0, has_side_effects=True, vmem_limit_bytes=67_043_328),
        )(x.reshape(8, rows // 8, dim), gain.reshape(1, dim), turn, wq, wk, wv, wo)
        fin = fin.astype(f32)
        first = lax.axis_index("tp") % 2 == 0
        total = jnp.concatenate([jnp.where(first, own, fin), jnp.where(first, fin, own)], 0)
        return (x.astype(f32) + total).astype(bf)

    tokens, columns = P(("dp", "tp"), None), P(None, "tp")
    return jax.shard_map(
        step,
        mesh=mesh,
        in_specs=(tokens, P(None), columns, columns, columns, P("tp", None)),
        out_specs=tokens,
        check_vma=False,
    )
```

```python
import functools

import jax
import jax.numpy as jnp
from jax import lax
from jax.experimental import pallas as pl
from jax.experimental.pallas import tpu as pltpu
from jax.sharding import PartitionSpec as P

HEAD = 128
THETA = 10000
NEG = -1e30
HIDDEN = 2 * NEG
LOG2E = 1.4426950408889634
CHIPS = 4
BLOCKS = 8
UNITS = 4
MESH = pl.DeviceIdType.MESH


def _dot(a, b, ca, cb):
    return lax.dot_general(a, b, (((ca,), (cb,)), ((), ())), preferred_element_type=jnp.float32)


QA = [262144, 798850, 1593668, 2658824, 3724044, 4789264, 5854484, 6391320, 262144, 794753, 1331460, 2396680, 3461900, 4260814, 4260880, 4260880, 0, 262144, 1331460, 2396680, 3724044, 4260880, 4260880, 4260880, 0, 0, 1331460, 2658824, 3724044, 4789264, 5854484, 6391320]
QR = [0, 0, 0, 1065216, 2130436, 3195656, 4260876, 5854544, 0, 0, 0, 0, 0, 0, 1855681, 3986250, 0, 0, 0, 0, 794688, 1859908, 3457738, 5051342, 0, 0, 0, 1065216, 2130436, 3195656, 4260876, 5326096]
TA = [8257, 16579, 29062, 45706, 62350, 78994, 95638, 99864, 24901, 41545, 45706, 49867, 58253, 66576, 66576, 66576, 24901, 41545, 62350, 66576, 66576, 66576, 66576, 66576, 24901, 41610, 58254, 78994, 95638, 99864, 99864, 99864]
TR = [0, 0, 0, 16644, 33288, 49932, 66576, 120278, 0, 0, 0, 0, 0, 4160, 41543, 78927, 0, 0, 16579, 33223, 37384, 41609, 58253, 99731, 0, 16644, 33288, 49932, 66576, 83220, 99860, 116440]
ORDER = [449161512, 656982510, 864803508, 102794106, 173013948, 230, 118571040, 677563538, 814471413, 430302537, 534213051, 1022, 172066848, 379887846, 864532908, 959301456, 1063211955, 758, 172066848, 379887846, 587708844, 795529842, 1003350840, 1022]


def _pick(table, at):
    got = 0
    for i, v in enumerate(table):
        got = got + jnp.where(at == i, v, 0)
    return got


def _field(word, n, bits=6):
    return lax.shift_right_logical(word, bits * n) & (2**bits - 1)


def _block(c, i):
    j = i - 2
    return jnp.where(c == 0, i, jnp.where(i < 2, 2 * c + i, jnp.where(j < 2 * c, j, i)))


def _ready(c, i):
    rest = jnp.where(i < 2, 0, jnp.where(i - 1 < 2 * c, i - 1, i + 1))
    return jnp.where(c == 0, i + 1, rest)


def layer(x_ref, gain_ref, turn_ref, wq_ref, wk_ref, wv_ref, wo_ref, sums, xg, own_s, sib_in,
          xv, gain_v, turn_v, wbuf, wobuf, acc, qv, kc, vt, ov, top_s, mix_s, tbuf, tst, rs_own, rs_sib, land,
          lsem, wsem, osem, tsem, tssem, recv_r, recv_l, recv_o, recv_s, send_r, send_l, send_o, send_s,
          recv_t, recv_rl, recv_rr, recv_f, out_sem, rsem, fsem):
    t = lax.axis_index("tp")
    c, k = t // 2, t % 2
    me, sib, left, right = {"tp": t}, {"tp": t + 1 - 2 * k}, {"tp": t - 2}, {"tp": t + 2}
    mine, other = 2 * c + k, 2 * c + 1 - k
    heads, rows = qv.shape[1], qv.shape[2]
    depth, width = wbuf.shape[2], wbuf.shape[3]
    steps = xv.shape[2] // depth
    wide = wobuf.shape[2]
    first, final = c == 0, c == CHIPS - 1

    def remote(src, dst, ssem, rsem, to):
        return pltpu.make_async_remote_copy(src_ref=src, dst_ref=dst, send_sem=ssem, recv_sem=rsem, device_id=to, device_id_type=MESH)

    def unit(b, h, j):
        return xg.at[(b * 2 + h) * UNITS + j]

    def to_right(b, j):
        u = unit(b, k, j)
        return remote(u, u, send_r.at[b * UNITS + j], recv_r.at[b * UNITS + j], right)

    def to_left(b, j):
        u = unit(b, k, j)
        return remote(u, u, send_l.at[b * UNITS + j], recv_l.at[b * UNITS + j], left)

    def to_sib(b, j):
        u = unit(b, k, j)
        return remote(u, u, send_s.at[b * UNITS + j], recv_s.at[b * UNITS + j], sib)

    def own_to_sib(h, j):
        u = unit(mine, h, j)
        return remote(u, u, send_o.at[h * UNITS + j], recv_o.at[h * UNITS + j], sib)

    def fetch_w(g):
        at, slot = pl.multiple_of((g % steps) * depth, depth), g % 3
        return [pltpu.make_async_copy(w.at[pl.ds(at, depth), :], wbuf.at[slot, i], wsem.at[slot, i])
                for i, w in enumerate((wq_ref, wk_ref, wv_ref))]

    def fetch_wo(j):
        return pltpu.make_async_copy(wo_ref.at[:, pl.ds(pl.multiple_of(j * wide, 128), wide)], wobuf.at[j % 2], osem.at[j % 2])

    barrier = pltpu.get_barrier_semaphore()
    pl.semaphore_signal(barrier, inc=1, device_id=sib, device_id_type=MESH)

    @pl.when(jnp.logical_not(first))
    def _():
        pl.semaphore_signal(barrier, inc=1, device_id=left, device_id_type=MESH)

    @pl.when(jnp.logical_not(final))
    def _():
        pl.semaphore_signal(barrier, inc=1, device_id=right, device_id_type=MESH)

    load_x = pltpu.make_async_copy(x_ref, xv, lsem.at[0])
    load_g = pltpu.make_async_copy(gain_ref, gain_v, lsem.at[1])
    load_x.start()
    load_g.start()
    for g in range(2):
        for cp in fetch_w(g):
            cp.start()
    load_x.wait()
    load_g.wait()

    def norm(n, _):
        at = (n // 2, pl.ds(pl.multiple_of((n % 2) * (xv.shape[1] // 2), xv.shape[1] // 2), xv.shape[1] // 2))
        wx = xv[at[0], at[1], :].astype(jnp.float32)
        scale = lax.rsqrt(jnp.mean(wx * wx, -1, keepdims=True) + 1e-6)
        xv[at[0], at[1], :] = (wx * scale * gain_v[...].astype(jnp.float32)).astype(jnp.bfloat16)

    lax.fori_loop(0, 16, norm, None)
    keep = pltpu.make_async_copy(xv, xg.at[pl.ds(mine * 8, 8)], lsem.at[0])
    keep.start()
    keep.wait()

    middle = jnp.logical_and(jnp.logical_not(first), jnp.logical_not(final))

    @pl.when(middle)
    def _():
        pl.semaphore_wait(barrier, 3)

    @pl.when(jnp.logical_not(middle))
    def _():
        pl.semaphore_wait(barrier, 2)

    for n in range(8):
        h = 1 - k if n < 4 else k
        own_to_sib(h, n % 4).start()

    def begin(i, _):
        b, j = 2 * c + i // UNITS, i % UNITS

        @pl.when(b == other)
        def _():
            u = unit(other, k, j)
            remote(u, u, send_o.at[k * UNITS + j], recv_o.at[k * UNITS + j], sib).wait_recv()

        @pl.when(jnp.logical_not(first))
        def _():
            to_left(b, j).start()

        @pl.when(first)
        def _():
            to_right(b, j).start()

    lax.fori_loop(0, 2 * UNITS, begin, None)
    for h in range(heads):
        vt[h, HEAD:, :] = jnp.ones((vt.shape[1] - HEAD, vt.shape[2]), jnp.bfloat16)

    def slot(i, _):
        j = i % UNITS

        @pl.when(i < 8 * c)
        def _():
            b = i // UNITS
            to_right(b, j).wait_recv()

            @pl.when(jnp.logical_not(final))
            def _():
                to_right(b, j).start()

            to_sib(b, j).start()

            @pl.when(jnp.logical_and(jnp.logical_not(final), i == 8 * c - 1))
            def _():
                def own(n, _):
                    to_right(2 * c + n // UNITS, n % UNITS).start()

                lax.fori_loop(0, 2 * UNITS, own, None)

        @pl.when(i < 8 * (CHIPS - 1 - c))
        def _():
            b = 2 * c + 2 + i // UNITS
            to_left(b, j).wait_recv()

            @pl.when(jnp.logical_not(first))
            def _():
                to_left(b, j).start()

            to_sib(b, j).start()

    def attend(b, place):
        e = HEAD**-0.5 * LOG2E
        top_s[...] = jnp.full(top_s.shape, NEG, jnp.float32)
        mix_s[...] = jnp.zeros(mix_s.shape, jnp.float32)

        def block(j, masked):
            here = pl.ds(pl.multiple_of(j * rows, rows), rows)
            scores = [_dot(kc[h, here, :], qv[place, h], 1, 1) for h in range(heads)]
            weights, keeps = [], []
            for h, s in enumerate(scores):
                if masked:
                    ok = lax.broadcasted_iota(jnp.int32, s.shape, 1) >= lax.broadcasted_iota(jnp.int32, s.shape, 0)
                    s = jnp.where(ok, s, HIDDEN)
                old = top_s[h : h + 1, :]
                top = jnp.maximum(old, s.max(axis=0, keepdims=True))
                top_s[h : h + 1, :] = top
                weights.append(jnp.exp2((s - top) * e).astype(jnp.bfloat16))
                keeps.append(jnp.exp2((old - top) * e))
            for h in range(heads):
                mix_s[h] = mix_s[h] * keeps[h] + _dot(vt[h, :, here], weights[h], 1, 0)

        lax.fori_loop(0, b, lambda j, _: block(j, False), None)
        block(b, True)
        for h in range(heads):
            total = mix_s[h, HEAD : HEAD + 1, :]
            ov[:, h * HEAD : (h + 1) * HEAD] = (mix_s[h, :HEAD, :] * (1 / total)).T.astype(jnp.bfloat16)

    def nth(r):
        u = _field(_pick(ORDER, c * 6 + r // 6), r % 6, 5)
        return u // UNITS, u % UNITS

    def loads(r, b, j):
        return [pltpu.make_async_copy(own_s.at[b, j], rs_own.at[r % 2], rsem.at[r % 2, 0]),
                pltpu.make_async_copy(sib_in.at[b, j], rs_sib.at[r % 2], rsem.at[r % 2, 1])]

    def ask(r):
        b, j = nth(r)
        remote(tst.at[0], sib_in.at[b, j], tssem.at[0], recv_t.at[b * UNITS + j], sib).wait_recv()
        for cp in loads(r, b, j):
            cp.start()

    def add(start, end):
        @pl.when(start < end)
        def _():
            ask(start)

        def one(r, _):
            @pl.when(r + 1 < end)
            def _():
                ask(r + 1)

            b, j = nth(r)
            d, p = b // 2, r % 2
            for cp in loads(r, b, j):
                cp.wait()
            rs_own[p] = rs_own[p] + rs_sib[p].astype(jnp.float32)

            @pl.when(jnp.logical_and(d >= c, jnp.logical_not(first)))
            def _():
                remote(land.at[b + 2, j], land.at[b + 2, j], out_sem.at[b * UNITS + j], recv_rl.at[b * UNITS + j], left).wait_recv()
                rs_own[p] = rs_own[p] + land[b + 2, j].astype(jnp.float32)

            @pl.when(jnp.logical_and(d <= c, jnp.logical_not(final)))
            def _():
                remote(land.at[b, j], land.at[b, j], out_sem.at[b * UNITS + j], recv_rr.at[b * UNITS + j], right).wait_recv()
                rs_own[p] = rs_own[p] + land[b, j].astype(jnp.float32)

            @pl.when(d > c)
            def _():
                land[b + 2, j] = rs_own[p].astype(jnp.bfloat16)
                remote(land.at[b + 2, j], land.at[b + 2, j], out_sem.at[b * UNITS + j], recv_rl.at[b * UNITS + j], right).start()

            @pl.when(d < c)
            def _():
                land[b, j] = rs_own[p].astype(jnp.bfloat16)
                remote(land.at[b, j], land.at[b, j], out_sem.at[b * UNITS + j], recv_rr.at[b * UNITS + j], left).start()

            result = sums.at[k, :, pl.ds(pl.multiple_of(j * wide, 128), wide)]

            @pl.when(b == mine)
            def _():
                cp = pltpu.make_async_copy(rs_own.at[p], result, fsem.at[0])
                cp.start()
                cp.wait()

            @pl.when(b == other)
            def _():
                cp = remote(rs_own.at[p], result, fsem.at[1], recv_f.at[j], sib)
                cp.start()
                cp.wait_send()

        lax.fori_loop(start, end, one, None)

    def work(i, _):
        b = _block(c, i)
        place = jnp.where(b // 2 == c, b % 2, 2)
        qa, qr = _pick(QA, c * BLOCKS + i), _pick(QR, c * BLOCKS + i)
        before = jnp.where(i == 0, 0, _field(_pick(TA, c * BLOCKS + _ready(c, i - 1) - 1), 2))
        before = jnp.where(jnp.logical_and(i > 0, _ready(c, i - 1) == _ready(c, i - 2)), _field(_pick(QA, c * BLOCKS + i - 1), 3), before)
        lax.fori_loop(before, _field(qa, 0), slot, None)

        @pl.when(b // 2 != c)
        def _():
            for j in range(UNITS):
                u = unit(b, 1 - k, j)
                remote(u, u, send_s.at[b * UNITS + j], recv_s.at[b * UNITS + j], sib).wait_recv()

        @pl.when(b == other)
        def _():
            for j in range(UNITS):
                u = unit(b, 1 - k, j)
                remote(u, u, send_o.at[j], recv_o.at[(1 - k) * UNITS + j], sib).wait_recv()

        tokens = pltpu.make_async_copy(xg.at[pl.ds(b * 8, 8)], xv, lsem.at[0])
        turns = pltpu.make_async_copy(turn_ref.at[:, b], turn_v, lsem.at[1])
        tokens.start()
        turns.start()
        acc[...] = jnp.zeros(acc.shape, jnp.float32)
        tokens.wait()
        turns.wait()

        def project(s, _):
            g = i * steps + s

            @pl.when(g + 2 < BLOCKS * steps)
            def _():
                for cp in fetch_w(g + 2):
                    cp.start()

            for cp in fetch_w(g):
                cp.wait()
            a = xv[:, :, pl.ds(pl.multiple_of(s * depth, 128), depth)].reshape(rows, depth)
            for m in range(3):
                acc[m] = acc[m] + jnp.dot(a, wbuf[g % 3, m], preferred_element_type=jnp.float32)

            @pl.when(jnp.logical_or(s == 4, jnp.logical_or(s == 9, s == 13)))
            def _():
                n = s // 5
                lax.fori_loop(_field(qa, n), _field(qa, n + 1), slot, None)
                add(_field(qr, n), _field(qr, n + 1))

        lax.fori_loop(0, steps, project, None)
        at = pl.ds(pl.multiple_of(b * rows, rows), rows)
        cos, sin = turn_v[0], turn_v[1]
        for h in range(heads):
            cols = slice(h * HEAD, (h + 1) * HEAD)
            q = acc[0, :, cols].astype(jnp.bfloat16).astype(jnp.float32)
            qv[place, h] = (q * cos + pltpu.roll(q, HEAD // 2, 1) * sin).astype(jnp.bfloat16)
            key = acc[1, :, cols].astype(jnp.bfloat16).astype(jnp.float32)
            kc[h, at, :] = (key * cos + pltpu.roll(key, HEAD // 2, 1) * sin).astype(jnp.bfloat16)
            vt[h, :HEAD, at] = acc[2, :, cols].T.astype(jnp.bfloat16)
        lax.fori_loop(jnp.where(i == 0, 0, _ready(c, i - 1)), _ready(c, i), finish, None)

    def finish(b, _):
        ta, tr = _pick(TA, c * BLOCKS + b), _pick(TR, c * BLOCKS + b)
        for j in range(2):
            fetch_wo(j).start()
        attend(b, jnp.where(b // 2 == c, b % 2, 2))
        lax.fori_loop(_field(ta, 0), _field(ta, 1), slot, None)
        add(_field(tr, 0), _field(tr, 1))

        def term(j, _):
            place = j % 2
            mine_out = pltpu.make_async_copy(tbuf.at[place, k], own_s.at[b, j], tsem.at[place])
            theirs_out = remote(tst.at[place], sib_in.at[b, j], tssem.at[place], recv_t.at[b * UNITS + j], sib)

            @pl.when(j >= 2)
            def _():
                mine_out.wait()
                theirs_out.wait_send()

            fetch_wo(j).wait()
            tbuf[place] = jnp.dot(ov[...], wobuf[place], preferred_element_type=jnp.float32).reshape(tbuf.shape[1:])

            @pl.when(j + 2 < UNITS)
            def _():
                fetch_wo(j + 2).start()

            tst[place] = tbuf[place, 1 - k].astype(jnp.bfloat16)
            mine_out.start()
            theirs_out.start()

        lax.fori_loop(0, UNITS, term, None)
        for place in range(2):
            pltpu.make_async_copy(tbuf.at[place, k], own_s.at[b, place], tsem.at[place]).wait()
            remote(tst.at[place], sib_in.at[b, place], tssem.at[place], recv_t.at[b * UNITS + place], sib).wait_send()
        lax.fori_loop(_field(ta, 1), _field(ta, 2), slot, None)
        add(_field(tr, 1), _field(tr, 2))

    lax.fori_loop(0, BLOCKS, work, None)
    add(_field(_pick(TR, c * BLOCKS + BLOCKS - 1), 2), BLOCKS * UNITS)

    for j in range(UNITS):
        remote(rs_own.at[0], sums.at[1 - k, :, pl.ds(j * wide, wide)], fsem.at[1], recv_f.at[j], sib).wait_recv()
    for n in range(8):
        own_to_sib(n // 4, n % 4).wait_send()

    def passed(i, _):
        b, j = i // UNITS, i % UNITS

        @pl.when(jnp.logical_and(jnp.logical_not(final), b <= 2 * c + 1))
        def _():
            to_right(b, j).wait_send()

        @pl.when(jnp.logical_and(jnp.logical_not(first), b >= 2 * c))
        def _():
            to_left(b, j).wait_send()

        @pl.when(b // 2 != c)
        def _():
            to_sib(b, j).wait_send()
            remote(land.at[b, j], land.at[b, j], out_sem.at[b * UNITS + j], recv_rr.at[b * UNITS + j], left).wait_send()

    lax.fori_loop(0, BLOCKS * UNITS, passed, None)


def turns(rows):
    half = HEAD // 2
    angle = jnp.arange(rows).astype(jnp.float32)[:, None] * THETA ** (-jnp.arange(half, dtype=jnp.float32) / half)
    cos, sin = jnp.cos(angle), jnp.sin(angle)
    return jnp.stack([jnp.concatenate([cos, cos], -1), jnp.concatenate([-sin, sin], -1)])


def solution(mesh):
    def step(x, gain, wq, wk, wv, wo):
        rows, dim = x.shape
        width = wq.shape[1]
        heads, half, wide, depth = width // HEAD, rows // 2, dim // UNITS, dim // 14
        bf, f32 = jnp.bfloat16, jnp.float32
        hbm = pl.BlockSpec(memory_space=pl.ANY)
        dma = pltpu.SemaphoreType.DMA
        turn = turns(BLOCKS * rows).reshape(2, BLOCKS, rows, HEAD)
        shape = jax.ShapeDtypeStruct
        total, *_ = pl.pallas_call(
            layer,
            out_shape=[
                shape((2, half, dim), f32),
                shape((BLOCKS * 8, rows // 8, dim), bf),
                shape((BLOCKS, UNITS, half, wide), f32),
                shape((BLOCKS, UNITS, half, wide), bf),
            ],
            in_specs=[hbm] * 7,
            out_specs=[hbm] * 4,
            scratch_shapes=[
                pltpu.VMEM((8, rows // 8, dim), bf),
                pltpu.VMEM((1, dim), bf),
                pltpu.VMEM((2, rows, HEAD), f32),
                pltpu.VMEM((3, 3, depth, width), bf),
                pltpu.VMEM((2, width, wide), bf),
                pltpu.VMEM((3, rows, width), f32),
                pltpu.VMEM((3, heads, rows, HEAD), bf),
                pltpu.VMEM((heads, BLOCKS * rows, HEAD), bf),
                pltpu.VMEM((heads, HEAD + 16, BLOCKS * rows), bf),
                pltpu.VMEM((rows, width), bf),
                pltpu.VMEM((heads, rows), f32),
                pltpu.VMEM((heads, HEAD + 16, rows), f32),
                pltpu.VMEM((2, 2, half, wide), f32),
                pltpu.VMEM((2, half, wide), bf),
                pltpu.VMEM((2, half, wide), f32),
                pltpu.VMEM((2, half, wide), bf),
                pltpu.VMEM((BLOCKS + 2, UNITS, half, wide), bf),
                dma((2,)), dma((3, 3)), dma((2,)), dma((2,)), dma((2,)),
                dma((24,)), dma((32,)), dma((8,)), dma((32,)),
                dma((32,)), dma((32,)), dma((8,)), dma((32,)),
                dma((32,)), dma((32,)), dma((32,)), dma((4,)), dma((32,)), dma((2, 2)), dma((2,)),
            ],
            compiler_params=pltpu.CompilerParams(collective_id=0, has_side_effects=True, vmem_limit_bytes=67_043_328),
        )(x.reshape(8, rows // 8, dim), gain.reshape(1, dim), turn, wq, wk, wv, wo)
        return (x.astype(f32) + total.reshape(rows, dim)).astype(bf)

    tokens, columns = P(("dp", "tp"), None), P(None, "tp")
    return jax.shard_map(
        step,
        mesh=mesh,
        in_specs=(tokens, P(None), columns, columns, columns, P("tp", None)),
        out_specs=tokens,
        check_vma=False,
    )
```

```python
import functools

import jax
import jax.numpy as jnp
from jax import lax
from jax.experimental import pallas as pl
from jax.experimental.pallas import tpu as pltpu
from jax.sharding import PartitionSpec as P

HEAD = 128
THETA = 10000
NEG = -1e30
HIDDEN = 2 * NEG
LOG2E = 1.4426950408889634
CHIPS = 4
BLOCKS = 8
UNITS = 4
MESH = pl.DeviceIdType.MESH


def _dot(a, b, ca, cb):
    return lax.dot_general(a, b, (((ca,), (cb,)), ((), ())), preferred_element_type=jnp.float32)


QA = [262144, 794753, 1331460, 2396680, 3461900, 4527120, 5592340, 6391320, 262144, 532545, 1331460, 2396680, 3457803, 3994510, 4260880, 4260880, 0, 262144, 1331460, 2662984, 3461900, 4260880, 4260880, 4260880, 0, 0, 1331460, 2396680, 3461900, 5059728, 5854548, 6391320]
QR = [0, 0, 0, 68174084, 119304647, 187478731, 255652815, 323826899, 0, 0, 0, 0, 0, 0, 85209153, 221033033, 0, 0, 0, 17039360, 68169858, 136343941, 238342924, 306516943, 0, 0, 0, 68174084, 136348168, 204522252, 272696336, 340870420]
TA = [4161, 12483, 24901, 41545, 58189, 74833, 91477, 99864, 24901, 41545, 41610, 45770, 58189, 66511, 66576, 66576, 24901, 45706, 58253, 66576, 66576, 66576, 66576, 66576, 24901, 41545, 58189, 83155, 95638, 99864, 99864, 99864]
TR = [0, 0, 16384, 28932, 45511, 62155, 78799, 95443, 0, 0, 0, 0, 0, 4096, 37317, 70605, 0, 8321, 20804, 37448, 45705, 49867, 62414, 79058, 16384, 33028, 49672, 66316, 82960, 99604, 99864, 99864]
ORDER = [449161512, 691619342, 899440341, 33519515, 172080193, 230, 86033424, 189943923, 864279766, 380479304, 501675420, 511, 172066848, 379887846, 864532908, 656993818, 770373276, 767, 172066848, 379887846, 587708844, 795529842, 1003350840, 1022]


def _pick(table, at):
    got = 0
    for i, v in enumerate(table):
        got = got + jnp.where(at == i, v, 0)
    return got


def _field(word, n, bits=6):
    return lax.shift_right_logical(word, bits * n) & (2**bits - 1)


def _block(c, i):
    j = i - 2
    return jnp.where(c == 0, i, jnp.where(i < 2, 2 * c + i, jnp.where(j < 2 * c, j, i)))


def _ready(c, i):
    rest = jnp.where(i < 2, 0, jnp.where(i - 1 < 2 * c, i - 1, i + 1))
    return jnp.where(c == 0, i + 1, rest)


def layer(x_ref, gain_ref, turn_ref, wq_ref, wk_ref, wv_ref, wo_ref, sums, xg, own_s, sib_in,
          xv, gain_v, turn_v, wbuf, wobuf, acc, qv, kc, vt, ov, top_s, mix_s, tbuf, tst, rs_own, rs_sib, land,
          base_v, row_v, xsem, ksem, lsem, wsem, osem, tsem, tssem, recv_r, recv_l, recv_o, recv_s, send_r, send_l, send_o, send_s,
          recv_t, recv_rl, recv_rr, recv_f, out_sem, rsem, fsem):
    t = lax.axis_index("tp")
    c, k = t // 2, t % 2
    me, sib, left, right = {"tp": t}, {"tp": t + 1 - 2 * k}, {"tp": t - 2}, {"tp": t + 2}
    mine, other = 2 * c + k, 2 * c + 1 - k
    heads, rows = qv.shape[1], qv.shape[2]
    depth, width = wbuf.shape[2], wbuf.shape[3]
    steps = xv.shape[2] // depth
    wide = wobuf.shape[2]
    first, final = c == 0, c == CHIPS - 1

    def remote(src, dst, ssem, rsem, to):
        return pltpu.make_async_remote_copy(src_ref=src, dst_ref=dst, send_sem=ssem, recv_sem=rsem, device_id=to, device_id_type=MESH)

    def unit(b, h, j):
        return xg.at[(b * 2 + h) * UNITS + j]

    def to_right(b, j):
        u = unit(b, k, j)
        return remote(u, u, send_r.at[b * UNITS + j], recv_r.at[b * UNITS + j], right)

    def to_left(b, j):
        u = unit(b, k, j)
        return remote(u, u, send_l.at[b * UNITS + j], recv_l.at[b * UNITS + j], left)

    def to_sib(b, j):
        u = unit(b, k, j)
        return remote(u, u, send_s.at[b * UNITS + j], recv_s.at[b * UNITS + j], sib)

    def own_to_sib(h, j):
        u = unit(mine, h, j)
        return remote(u, u, send_o.at[h * UNITS + j], recv_o.at[h * UNITS + j], sib)

    def fetch_w(g):
        at, slot = pl.multiple_of((g % steps) * depth, depth), g % 3
        return [pltpu.make_async_copy(w.at[pl.ds(at, depth), :], wbuf.at[slot, i], wsem.at[slot, i])
                for i, w in enumerate((wq_ref, wk_ref, wv_ref))]

    def fetch_wo(j):
        return pltpu.make_async_copy(wo_ref.at[:, pl.ds(pl.multiple_of(j * wide, 128), wide)], wobuf.at[j % 2], osem.at[j % 2])

    barrier = pltpu.get_barrier_semaphore()
    pl.semaphore_signal(barrier, inc=1, device_id=sib, device_id_type=MESH)

    @pl.when(jnp.logical_not(first))
    def _():
        pl.semaphore_signal(barrier, inc=1, device_id=left, device_id_type=MESH)

    @pl.when(jnp.logical_not(final))
    def _():
        pl.semaphore_signal(barrier, inc=1, device_id=right, device_id_type=MESH)

    def half_of(n):
        return jnp.where(n % 2 == 0, 1 - k, k)

    def load_x(n):
        u = half_of(n) * UNITS + n // 2
        return pltpu.make_async_copy(x_ref.at[u], xv.at[u], xsem.at[n])

    def keep_x(n):
        u = half_of(n) * UNITS + n // 2
        return pltpu.make_async_copy(xv.at[u], xg.at[mine * 8 + u], ksem.at[n])

    load_g = pltpu.make_async_copy(gain_ref, gain_v, lsem.at[0])
    load_t = pltpu.make_async_copy(turn_ref, base_v, lsem.at[1])
    load_g.start()
    for n in range(8):
        load_x(n).start()
    load_t.start()
    for g in range(2):
        for cp in fetch_w(g):
            cp.start()
    load_g.wait()
    for n in range(gain_v.shape[0]):
        row_v[:, n * HEAD : (n + 1) * HEAD] = gain_v[n : n + 1, :].astype(jnp.float32)

    middle = jnp.logical_and(jnp.logical_not(first), jnp.logical_not(final))

    @pl.when(middle)
    def _():
        pl.semaphore_wait(barrier, 3)

    @pl.when(jnp.logical_not(middle))
    def _():
        pl.semaphore_wait(barrier, 2)

    def link(b, j, i):
        @pl.when(jnp.logical_not(first))
        def _():
            to_left(b, j).start()

        @pl.when(jnp.logical_or(first, jnp.logical_and(jnp.logical_not(final), i < c)))
        def _():
            to_right(b, j).start()

    def norm(n, _):
        @pl.when(n < 8)
        def _():
            u, some = half_of(n) * UNITS + n // 2, xv.shape[1] // 2
            load_x(n).wait()
            for m in range(2):
                here = slice(m * some, (m + 1) * some)
                wx = xv[u, here, :].astype(jnp.float32)
                scale = lax.rsqrt(jnp.mean(wx * wx, -1, keepdims=True) + 1e-6)
                xv[u, here, :] = (wx * scale * row_v[...]).astype(jnp.bfloat16)
            keep_x(n).start()

        @pl.when(n > 0)
        def _():
            h, j = half_of(n - 1), (n - 1) // 2
            keep_x(n - 1).wait()
            own_to_sib(h, j).start()

            @pl.when(jnp.logical_and(h == k, k == 0))
            def _():
                link(mine, j, j)

    lax.fori_loop(0, 9, norm, None)

    def begin(i, _):
        b, j = 2 * c + i // UNITS, i % UNITS

        @pl.when(b == other)
        def _():
            u = unit(other, k, j)
            remote(u, u, send_o.at[k * UNITS + j], recv_o.at[k * UNITS + j], sib).wait_recv()

        link(b, j, i)

    lax.fori_loop(UNITS * (1 - k), 2 * UNITS, begin, None)
    load_t.wait()
    for h in range(heads):
        vt[h, HEAD:, :] = jnp.ones((vt.shape[1] - HEAD, vt.shape[2]), jnp.bfloat16)

    def slot(i, _):
        j = i % UNITS

        @pl.when(i < 8 * c)
        def _():
            b = i // UNITS
            to_right(b, j).wait_recv()

            @pl.when(jnp.logical_not(final))
            def _():
                to_right(b, j).start()

            to_sib(b, j).start()

            @pl.when(jnp.logical_and(jnp.logical_not(final), i == 8 * c - 1))
            def _():
                def own(n, _):
                    to_right(2 * c + n // UNITS, n % UNITS).start()

                lax.fori_loop(c, 2 * UNITS, own, None)

        @pl.when(i < 8 * (CHIPS - 1 - c))
        def _():
            b = 2 * c + 2 + i // UNITS
            to_left(b, j).wait_recv()

            @pl.when(jnp.logical_not(first))
            def _():
                to_left(b, j).start()

            to_sib(b, j).start()

    def attend(b, place):
        e = HEAD**-0.5 * LOG2E
        top_s[...] = jnp.full(top_s.shape, NEG, jnp.float32)
        mix_s[...] = jnp.zeros(mix_s.shape, jnp.float32)

        def block(j, masked):
            here = pl.ds(pl.multiple_of(j * rows, rows), rows)
            scores = [_dot(kc[h, here, :], qv[place, h], 1, 1) for h in range(heads)]
            weights, keeps = [], []
            for h, s in enumerate(scores):
                if masked:
                    ok = lax.broadcasted_iota(jnp.int32, s.shape, 1) >= lax.broadcasted_iota(jnp.int32, s.shape, 0)
                    s = jnp.where(ok, s, HIDDEN)
                old = top_s[h : h + 1, :]
                top = jnp.maximum(old, s.max(axis=0, keepdims=True))
                top_s[h : h + 1, :] = top
                weights.append(jnp.exp2((s - top) * e).astype(jnp.bfloat16))
                keeps.append(jnp.exp2((old - top) * e))
            for h in range(heads):
                mix_s[h] = mix_s[h] * keeps[h] + _dot(vt[h, :, here], weights[h], 1, 0)

        lax.fori_loop(0, b, lambda j, _: block(j, False), None)
        block(b, True)
        for h in range(heads):
            total = mix_s[h, HEAD : HEAD + 1, :]
            ov[:, h * HEAD : (h + 1) * HEAD] = (mix_s[h, :HEAD, :] * (1 / total)).T.astype(jnp.bfloat16)

    def nth(r):
        u = _field(_pick(ORDER, c * 6 + r // 6), r % 6, 5)
        return u // UNITS, u % UNITS

    def loads(r, b, j):
        return [pltpu.make_async_copy(own_s.at[b, j], rs_own.at[r % 2], rsem.at[r % 2, 0]),
                pltpu.make_async_copy(sib_in.at[b, j], rs_sib.at[r % 2], rsem.at[r % 2, 1])]

    def ask(r):
        b, j = nth(r)
        remote(tst.at[0], sib_in.at[b, j], tssem.at[0], recv_t.at[b * UNITS + j], sib).wait_recv()
        for cp in loads(r, b, j):
            cp.start()

    def add(start, end):
        @pl.when(start < end)
        def _():
            ask(start)

        def one(r, _):
            @pl.when(r + 1 < end)
            def _():
                ask(r + 1)

            b, j = nth(r)
            d, p = b // 2, r % 2
            for cp in loads(r, b, j):
                cp.wait()
            rs_own[p] = rs_own[p] + rs_sib[p].astype(jnp.float32)

            @pl.when(jnp.logical_and(d >= c, jnp.logical_not(first)))
            def _():
                remote(land.at[b + 2, j], land.at[b + 2, j], out_sem.at[b * UNITS + j], recv_rl.at[b * UNITS + j], left).wait_recv()
                rs_own[p] = rs_own[p] + land[b + 2, j].astype(jnp.float32)

            @pl.when(jnp.logical_and(d <= c, jnp.logical_not(final)))
            def _():
                remote(land.at[b, j], land.at[b, j], out_sem.at[b * UNITS + j], recv_rr.at[b * UNITS + j], right).wait_recv()
                rs_own[p] = rs_own[p] + land[b, j].astype(jnp.float32)

            @pl.when(d > c)
            def _():
                land[b + 2, j] = rs_own[p].astype(jnp.bfloat16)
                remote(land.at[b + 2, j], land.at[b + 2, j], out_sem.at[b * UNITS + j], recv_rl.at[b * UNITS + j], right).start()

            @pl.when(d < c)
            def _():
                land[b, j] = rs_own[p].astype(jnp.bfloat16)
                remote(land.at[b, j], land.at[b, j], out_sem.at[b * UNITS + j], recv_rr.at[b * UNITS + j], left).start()

            result = sums.at[k, :, pl.ds(pl.multiple_of(j * wide, 128), wide)]

            @pl.when(b == mine)
            def _():
                cp = pltpu.make_async_copy(rs_own.at[p], result, fsem.at[0])
                cp.start()
                cp.wait()

            @pl.when(b == other)
            def _():
                cp = remote(rs_own.at[p], result, fsem.at[1], recv_f.at[j], sib)
                cp.start()
                cp.wait_send()

        lax.fori_loop(start, end, one, None)

    def work(i, _):
        b = _block(c, i)
        place = jnp.where(b // 2 == c, b % 2, 2)
        qa, qr = _pick(QA, c * BLOCKS + i), _pick(QR, c * BLOCKS + i)
        before = jnp.where(i == 0, 0, _field(_pick(TA, c * BLOCKS + _ready(c, i - 1) - 1), 2))
        before = jnp.where(jnp.logical_and(i > 0, _ready(c, i - 1) == _ready(c, i - 2)), _field(_pick(QA, c * BLOCKS + i - 1), 3), before)
        add(_field(qr, 0), _field(qr, 1))
        lax.fori_loop(before, _field(qa, 0), slot, None)

        @pl.when(b // 2 != c)
        def _():
            for j in range(UNITS):
                u = unit(b, 1 - k, j)
                remote(u, u, send_s.at[b * UNITS + j], recv_s.at[b * UNITS + j], sib).wait_recv()

        @pl.when(b == other)
        def _():
            for j in range(UNITS):
                u = unit(b, 1 - k, j)
                remote(u, u, send_o.at[j], recv_o.at[(1 - k) * UNITS + j], sib).wait_recv()

        tokens = pltpu.make_async_copy(xg.at[pl.ds(b * 8, 8)], xv, lsem.at[0])
        tokens.start()
        cos, sin = base_v[0, pl.ds(rows + b, 1), :], base_v[1, pl.ds(rows + b, 1), :]
        turn_v[0] = cos * base_v[0, :rows, :] - sin * base_v[1, :rows, :]
        turn_v[1] = sin * base_v[0, :rows, :] + cos * base_v[1, :rows, :]
        acc[...] = jnp.zeros(acc.shape, jnp.float32)
        tokens.wait()

        def project(s, _):
            g = i * steps + s

            @pl.when(g + 2 < BLOCKS * steps)
            def _():
                for cp in fetch_w(g + 2):
                    cp.start()

            for cp in fetch_w(g):
                cp.wait()
            a = xv[:, :, pl.ds(pl.multiple_of(s * depth, 128), depth)].reshape(rows, depth)
            for m in range(3):
                acc[m] = acc[m] + jnp.dot(a, wbuf[g % 3, m], preferred_element_type=jnp.float32)

            @pl.when(jnp.logical_or(s == 4, jnp.logical_or(s == 9, s == 13)))
            def _():
                n = s // 5
                lax.fori_loop(_field(qa, n), _field(qa, n + 1), slot, None)
                add(_field(qr, n + 1), _field(qr, n + 2))

        lax.fori_loop(0, steps, project, None)
        at = pl.ds(pl.multiple_of(b * rows, rows), rows)
        cos, sin = turn_v[0], turn_v[1]
        for h in range(heads):
            cols = slice(h * HEAD, (h + 1) * HEAD)
            q = acc[0, :, cols].astype(jnp.bfloat16).astype(jnp.float32)
            qv[place, h] = (q * cos + pltpu.roll(q, HEAD // 2, 1) * sin).astype(jnp.bfloat16)
            key = acc[1, :, cols].astype(jnp.bfloat16).astype(jnp.float32)
            kc[h, at, :] = (key * cos + pltpu.roll(key, HEAD // 2, 1) * sin).astype(jnp.bfloat16)
            vt[h, :HEAD, at] = acc[2, :, cols].T.astype(jnp.bfloat16)
        lax.fori_loop(jnp.where(i == 0, 0, _ready(c, i - 1)), _ready(c, i), finish, None)

    def finish(b, _):
        ta, tr = _pick(TA, c * BLOCKS + b), _pick(TR, c * BLOCKS + b)
        for j in range(2):
            fetch_wo(j).start()
        attend(b, jnp.where(b // 2 == c, b % 2, 2))
        lax.fori_loop(_field(ta, 0), _field(ta, 1), slot, None)
        add(_field(tr, 0), _field(tr, 1))

        def term(j, _):
            place = j % 2
            mine_out = pltpu.make_async_copy(tbuf.at[place, k], own_s.at[b, j], tsem.at[place])
            theirs_out = remote(tst.at[place], sib_in.at[b, j], tssem.at[place], recv_t.at[b * UNITS + j], sib)

            @pl.when(j >= 2)
            def _():
                mine_out.wait()
                theirs_out.wait_send()

            fetch_wo(j).wait()
            tbuf[place] = jnp.dot(ov[...], wobuf[place], preferred_element_type=jnp.float32).reshape(tbuf.shape[1:])

            @pl.when(j + 2 < UNITS)
            def _():
                fetch_wo(j + 2).start()

            tst[place] = tbuf[place, 1 - k].astype(jnp.bfloat16)
            mine_out.start()
            theirs_out.start()

        lax.fori_loop(0, UNITS, term, None)
        for place in range(2):
            pltpu.make_async_copy(tbuf.at[place, k], own_s.at[b, place], tsem.at[place]).wait()
            remote(tst.at[place], sib_in.at[b, place], tssem.at[place], recv_t.at[b * UNITS + place], sib).wait_send()
        lax.fori_loop(_field(ta, 1), _field(ta, 2), slot, None)
        add(_field(tr, 1), _field(tr, 2))

    lax.fori_loop(0, BLOCKS, work, None)
    add(_field(_pick(TR, c * BLOCKS + BLOCKS - 1), 2), BLOCKS * UNITS)

    for j in range(UNITS):
        remote(rs_own.at[0], sums.at[1 - k, :, pl.ds(j * wide, wide)], fsem.at[1], recv_f.at[j], sib).wait_recv()
    for n in range(8):
        own_to_sib(n // 4, n % 4).wait_send()

    def passed(i, _):
        b, j = i // UNITS, i % UNITS

        @pl.when(jnp.logical_and(jnp.logical_not(final), b <= 2 * c + 1))
        def _():
            to_right(b, j).wait_send()

        @pl.when(jnp.logical_and(jnp.logical_not(first), b >= 2 * c))
        def _():
            to_left(b, j).wait_send()

        @pl.when(b // 2 != c)
        def _():
            to_sib(b, j).wait_send()
            remote(land.at[b, j], land.at[b, j], out_sem.at[b * UNITS + j], recv_rr.at[b * UNITS + j], left).wait_send()

    lax.fori_loop(0, BLOCKS * UNITS, passed, None)


def turns(rows):
    lane, at = jnp.arange(HEAD), jnp.arange(rows + BLOCKS)
    place = jnp.where(at < rows, at, (at - rows) * rows)
    half = HEAD // 2
    angle = place.astype(jnp.float32)[:, None] * THETA ** (-(lane % half).astype(jnp.float32) / half)
    return jnp.stack([jnp.cos(angle), jnp.where(lane < half, -1.0, 1.0) * jnp.sin(angle)])


def solution(mesh):
    def step(x, gain, wq, wk, wv, wo):
        rows, dim = x.shape
        width = wq.shape[1]
        heads, half, wide, depth = width // HEAD, rows // 2, dim // UNITS, dim // 14
        bf, f32 = jnp.bfloat16, jnp.float32
        hbm = pl.BlockSpec(memory_space=pl.ANY)
        dma = pltpu.SemaphoreType.DMA
        turn = turns(rows)
        shape = jax.ShapeDtypeStruct
        total, *_ = pl.pallas_call(
            layer,
            out_shape=[
                shape((2, half, dim), f32),
                shape((BLOCKS * 8, rows // 8, dim), bf),
                shape((BLOCKS, UNITS, half, wide), f32),
                shape((BLOCKS, UNITS, half, wide), bf),
            ],
            in_specs=[hbm] * 7,
            out_specs=[hbm] * 4,
            scratch_shapes=[
                pltpu.VMEM((8, rows // 8, dim), bf),
                pltpu.VMEM((dim // HEAD, HEAD), bf),
                pltpu.VMEM((2, rows, HEAD), f32),
                pltpu.VMEM((3, 3, depth, width), bf),
                pltpu.VMEM((2, width, wide), bf),
                pltpu.VMEM((3, rows, width), f32),
                pltpu.VMEM((3, heads, rows, HEAD), bf),
                pltpu.VMEM((heads, BLOCKS * rows, HEAD), bf),
                pltpu.VMEM((heads, HEAD + 16, BLOCKS * rows), bf),
                pltpu.VMEM((rows, width), bf),
                pltpu.VMEM((heads, rows), f32),
                pltpu.VMEM((heads, HEAD + 16, rows), f32),
                pltpu.VMEM((2, 2, half, wide), f32),
                pltpu.VMEM((2, half, wide), bf),
                pltpu.VMEM((2, half, wide), f32),
                pltpu.VMEM((2, half, wide), bf),
                pltpu.VMEM((BLOCKS + 2, UNITS, half, wide), bf),
                pltpu.VMEM((2, rows + BLOCKS, HEAD), f32),
                pltpu.VMEM((1, dim), f32),
                dma((8,)), dma((8,)), dma((2,)), dma((3, 3)), dma((2,)), dma((2,)), dma((2,)),
                dma((24,)), dma((32,)), dma((8,)), dma((32,)),
                dma((32,)), dma((32,)), dma((8,)), dma((32,)),
                dma((32,)), dma((32,)), dma((32,)), dma((4,)), dma((32,)), dma((2, 2)), dma((2,)),
            ],
            compiler_params=pltpu.CompilerParams(collective_id=0, has_side_effects=True, vmem_limit_bytes=67_043_328),
        )(x.reshape(8, rows // 8, dim), gain.reshape(dim // HEAD, HEAD), turn, wq, wk, wv, wo)
        return (x.astype(f32) + total.reshape(rows, dim)).astype(bf)

    tokens, columns = P(("dp", "tp"), None), P(None, "tp")
    return jax.shard_map(
        step,
        mesh=mesh,
        in_specs=(tokens, P(None), columns, columns, columns, P("tp", None)),
        out_specs=tokens,
        check_vma=False,
    )
```

```python
import functools

import jax
import jax.numpy as jnp
from jax import lax
from jax.experimental import pallas as pl
from jax.experimental.pallas import tpu as pltpu
from jax.sharding import PartitionSpec as P

HEAD = 128
THETA = 10000
NEG = -1e30
HIDDEN = 2 * NEG
LOG2E = 1.4426950408889634
CHIPS = 4
BLOCKS = 8
UNITS = 4
MESH = pl.DeviceIdType.MESH


def _dot(a, b, ca, cb):
    return lax.dot_general(a, b, (((ca,), (cb,)), ((), ())), preferred_element_type=jnp.float32)


QA = [266240, 1061058, 1597764, 2658824, 3461900, 4527120, 5592340, 6391320, 266240, 794753, 1331460, 2396680, 3724108, 4260815, 4260880, 4260880, 0, 266240, 1331460, 2662984, 3724044, 4260880, 4260880, 4260880, 0, 0, 1331460, 2396680, 3461900, 5059728, 6120852, 6391320]
QR = [0, 0, 0, 68174084, 119304647, 187478731, 255652815, 323826899, 0, 0, 0, 0, 0, 50593792, 187203909, 306516943, 0, 0, 0, 16777216, 68169858, 136081733, 238342859, 323822673, 0, 0, 0, 68174084, 136348168, 204522252, 272696336, 340870420]
TA = [8257, 16644, 29126, 41610, 58253, 74897, 91541, 99864, 24965, 41609, 45706, 49867, 62350, 66576, 66576, 66576, 24965, 45770, 62350, 66576, 66576, 66576, 66576, 66576, 24901, 41609, 58253, 83219, 99799, 99864, 99864, 99864]
TR = [0, 0, 16384, 28932, 45511, 62155, 78799, 95443, 0, 0, 0, 0, 0, 20803, 62283, 83154, 0, 8257, 20804, 37384, 41609, 45770, 70606, 87315, 16384, 33028, 49672, 66316, 82960, 99604, 99864, 99864]
ORDER = [449161512, 691619342, 899440341, 33519515, 183635009, 230, 86033424, 189944419, 864279766, 345908090, 484389245, 511, 172066848, 379887846, 855390636, 588182394, 726650462, 758, 172066848, 379887846, 587708844, 795529842, 1003350840, 1022]


def _pick(table, at):
    got = 0
    for i, v in enumerate(table):
        got = got + jnp.where(at == i, v, 0)
    return got


def _field(word, n, bits=6):
    return lax.shift_right_logical(word, bits * n) & (2**bits - 1)


def _block(c, i):
    j = i - 2
    return jnp.where(c == 0, i, jnp.where(i < 2, 2 * c + i, jnp.where(j < 2 * c, j, i)))


def _ready(c, i):
    rest = jnp.where(i < 2, 0, jnp.where(i - 1 < 2 * c, i - 1, i + 1))
    return jnp.where(c == 0, i + 1, rest)


def layer(x_ref, gain_ref, turn_ref, wq_ref, wk_ref, wv_ref, wo_ref, sums, xg, own_s, sib_in,
          xv, gain_v, turn_v, wbuf, wobuf, acc, qv, kc, vt, ov, top_s, mix_s, tbuf, tst, rs_own, rs_sib, land,
          base_v, row_v, xsem, ksem, lsem, wsem, osem, tsem, tssem, recv_r, recv_l, recv_o, recv_s, send_r, send_l, send_o, send_s,
          recv_t, recv_rl, recv_rr, recv_f, out_sem, rsem, fsem):
    t = lax.axis_index("tp")
    c, k = t // 2, t % 2
    me, sib, left, right = {"tp": t}, {"tp": t + 1 - 2 * k}, {"tp": t - 2}, {"tp": t + 2}
    mine, other = 2 * c + k, 2 * c + 1 - k
    heads, rows = qv.shape[1], qv.shape[2]
    depth, width = wbuf.shape[2], wbuf.shape[3]
    steps = xv.shape[2] // depth
    wide = wobuf.shape[2]
    first, final = c == 0, c == CHIPS - 1

    def remote(src, dst, ssem, rsem, to):
        return pltpu.make_async_remote_copy(src_ref=src, dst_ref=dst, send_sem=ssem, recv_sem=rsem, device_id=to, device_id_type=MESH)

    def unit(b, h, j):
        return xg.at[(b * 2 + h) * UNITS + j]

    def to_right(b, j):
        u = unit(b, k, j)
        return remote(u, u, send_r.at[b * UNITS + j], recv_r.at[b * UNITS + j], right)

    def to_left(b, j):
        u = unit(b, k, j)
        return remote(u, u, send_l.at[b * UNITS + j], recv_l.at[b * UNITS + j], left)

    def to_sib(b, j):
        u = unit(b, k, j)
        return remote(u, u, send_s.at[b * UNITS + j], recv_s.at[b * UNITS + j], sib)

    def own_to_sib(h, j):
        u = unit(mine, h, j)
        return remote(u, u, send_o.at[h * UNITS + j], recv_o.at[h * UNITS + j], sib)

    def fetch_w(g):
        at, slot = pl.multiple_of((g % steps) * depth, depth), g % 3
        return [pltpu.make_async_copy(w.at[pl.ds(at, depth), :], wbuf.at[slot, i], wsem.at[slot, i])
                for i, w in enumerate((wq_ref, wk_ref, wv_ref))]

    def fetch_wo(j):
        return pltpu.make_async_copy(wo_ref.at[:, pl.ds(pl.multiple_of(j * wide, 128), wide)], wobuf.at[j % 2], osem.at[j % 2])

    barrier = pltpu.get_barrier_semaphore()
    pl.semaphore_signal(barrier, inc=1, device_id=sib, device_id_type=MESH)

    @pl.when(jnp.logical_not(first))
    def _():
        pl.semaphore_signal(barrier, inc=1, device_id=left, device_id_type=MESH)

    @pl.when(jnp.logical_not(final))
    def _():
        pl.semaphore_signal(barrier, inc=1, device_id=right, device_id_type=MESH)

    def half_of(n):
        return jnp.where(n % 2 == 0, 1 - k, k)

    def load_x(n):
        u = half_of(n) * UNITS + n // 2
        return pltpu.make_async_copy(x_ref.at[u], xv.at[u], xsem.at[n])

    def keep_x(n):
        u = half_of(n) * UNITS + n // 2
        return pltpu.make_async_copy(xv.at[u], xg.at[mine * 8 + u], ksem.at[n])

    load_g = pltpu.make_async_copy(gain_ref, gain_v, lsem.at[0])
    load_t = pltpu.make_async_copy(turn_ref, base_v, lsem.at[1])
    load_g.start()
    for n in range(8):
        load_x(n).start()
    load_t.start()
    for g in range(2):
        for cp in fetch_w(g):
            cp.start()
    load_g.wait()
    for n in range(gain_v.shape[0]):
        row_v[:, n * HEAD : (n + 1) * HEAD] = gain_v[n : n + 1, :].astype(jnp.float32)

    middle = jnp.logical_and(jnp.logical_not(first), jnp.logical_not(final))

    @pl.when(middle)
    def _():
        pl.semaphore_wait(barrier, 3)

    @pl.when(jnp.logical_not(middle))
    def _():
        pl.semaphore_wait(barrier, 2)

    def link(b, j, i):
        @pl.when(jnp.logical_not(first))
        def _():
            to_left(b, j).start()

        @pl.when(jnp.logical_or(first, jnp.logical_and(jnp.logical_not(final), i < 1 * c)))
        def _():
            to_right(b, j).start()

    def norm(n, _):
        @pl.when(n < 8)
        def _():
            u, some = half_of(n) * UNITS + n // 2, xv.shape[1] // 2
            load_x(n).wait()
            for m in range(2):
                here = slice(m * some, (m + 1) * some)
                wx = xv[u, here, :].astype(jnp.float32)
                scale = lax.rsqrt(jnp.mean(wx * wx, -1, keepdims=True) + 1e-6)
                xv[u, here, :] = (wx * scale * row_v[...]).astype(jnp.bfloat16)
            keep_x(n).start()

        @pl.when(n > 0)
        def _():
            h, j = half_of(n - 1), (n - 1) // 2
            keep_x(n - 1).wait()
            own_to_sib(h, j).start()

            @pl.when(jnp.logical_and(h == k, k == 0))
            def _():
                link(mine, j, j)

    lax.fori_loop(0, 9, norm, None)

    def begin(i, _):
        b, j = 2 * c + i // UNITS, i % UNITS

        @pl.when(b == other)
        def _():
            u = unit(other, k, j)
            remote(u, u, send_o.at[k * UNITS + j], recv_o.at[k * UNITS + j], sib).wait_recv()

        link(b, j, i)

    lax.fori_loop(UNITS * (1 - k), 2 * UNITS, begin, None)
    load_t.wait()
    for h in range(heads):
        vt[h, HEAD:, :] = jnp.ones((vt.shape[1] - HEAD, vt.shape[2]), jnp.bfloat16)

    def slot(i, _):
        j = i % UNITS

        @pl.when(i < 8 * c)
        def _():
            b = i // UNITS
            to_right(b, j).wait_recv()

            @pl.when(jnp.logical_not(final))
            def _():
                to_right(b, j).start()

            to_sib(b, j).start()

            @pl.when(jnp.logical_and(jnp.logical_not(final), i == 8 * c - 1))
            def _():
                def own(n, _):
                    to_right(2 * c + n // UNITS, n % UNITS).start()

                lax.fori_loop(1 * c, 2 * UNITS, own, None)

        @pl.when(i < 8 * (CHIPS - 1 - c))
        def _():
            b = 2 * c + 2 + i // UNITS
            to_left(b, j).wait_recv()

            @pl.when(jnp.logical_not(first))
            def _():
                to_left(b, j).start()

            to_sib(b, j).start()

    def attend(b, place):
        e = HEAD**-0.5 * LOG2E
        top_s[...] = jnp.full(top_s.shape, NEG, jnp.float32)
        mix_s[...] = jnp.zeros(mix_s.shape, jnp.float32)

        def block(j, masked):
            here = pl.ds(pl.multiple_of(j * rows, rows), rows)
            scores = [_dot(kc[h, here, :], qv[place, h], 1, 1) for h in range(heads)]
            weights, keeps = [], []
            for h, s in enumerate(scores):
                if masked:
                    ok = lax.broadcasted_iota(jnp.int32, s.shape, 1) >= lax.broadcasted_iota(jnp.int32, s.shape, 0)
                    s = jnp.where(ok, s, HIDDEN)
                old = top_s[h : h + 1, :]
                top = jnp.maximum(old, s.max(axis=0, keepdims=True))
                top_s[h : h + 1, :] = top
                weights.append(jnp.exp2((s - top) * e).astype(jnp.bfloat16))
                keeps.append(jnp.exp2((old - top) * e))
            for h in range(heads):
                mix_s[h] = mix_s[h] * keeps[h] + _dot(vt[h, :, here], weights[h], 1, 0)

        lax.fori_loop(0, b, lambda j, _: block(j, False), None)
        block(b, True)
        for h in range(heads):
            total = mix_s[h, HEAD : HEAD + 1, :]
            ov[:, h * HEAD : (h + 1) * HEAD] = (mix_s[h, :HEAD, :] * (1 / total)).T.astype(jnp.bfloat16)

    def nth(r):
        u = _field(_pick(ORDER, c * 6 + r // 6), r % 6, 5)
        return u // UNITS, u % UNITS

    def loads(r, b, j):
        return [pltpu.make_async_copy(own_s.at[b, j], rs_own.at[r % 2], rsem.at[r % 2, 0]),
                pltpu.make_async_copy(sib_in.at[b, j], rs_sib.at[r % 2], rsem.at[r % 2, 1])]

    def ask(r):
        b, j = nth(r)
        remote(tst.at[0], sib_in.at[b, j], tssem.at[0], recv_t.at[b * UNITS + j], sib).wait_recv()
        for cp in loads(r, b, j):
            cp.start()

    def add(start, end):
        @pl.when(start < end)
        def _():
            ask(start)

        def one(r, _):
            @pl.when(r + 1 < end)
            def _():
                ask(r + 1)

            b, j = nth(r)
            d, p = b // 2, r % 2
            for cp in loads(r, b, j):
                cp.wait()
            for q in range(2):
                some = pl.ds(q * (rs_own.shape[1] // 2), rs_own.shape[1] // 2)
                at = (b * UNITS + j) * 2 + q
                high, low = land.at[b + 2, j, some], land.at[b, j, some]
                rs_own[p, some] = rs_own[p, some] + rs_sib[p, some].astype(jnp.float32)

                @pl.when(jnp.logical_and(d >= c, jnp.logical_not(first)))
                def _():
                    remote(high, high, out_sem.at[at], recv_rl.at[at], left).wait_recv()
                    rs_own[p, some] = rs_own[p, some] + high[...].astype(jnp.float32)

                @pl.when(jnp.logical_and(d <= c, jnp.logical_not(final)))
                def _():
                    remote(low, low, out_sem.at[at], recv_rr.at[at], right).wait_recv()
                    rs_own[p, some] = rs_own[p, some] + low[...].astype(jnp.float32)

                @pl.when(d > c)
                def _():
                    high[...] = rs_own[p, some].astype(jnp.bfloat16)
                    remote(high, high, out_sem.at[at], recv_rl.at[at], right).start()

                @pl.when(d < c)
                def _():
                    low[...] = rs_own[p, some].astype(jnp.bfloat16)
                    remote(low, low, out_sem.at[at], recv_rr.at[at], left).start()

            result = sums.at[k, :, pl.ds(pl.multiple_of(j * wide, 128), wide)]

            @pl.when(b == mine)
            def _():
                cp = pltpu.make_async_copy(rs_own.at[p], result, fsem.at[0])
                cp.start()
                cp.wait()

            @pl.when(b == other)
            def _():
                cp = remote(rs_own.at[p], result, fsem.at[1], recv_f.at[j], sib)
                cp.start()
                cp.wait_send()

        lax.fori_loop(start, end, one, None)

    def work(i, _):
        b = _block(c, i)
        place = jnp.where(b // 2 == c, b % 2, 2)
        qa, qr = _pick(QA, c * BLOCKS + i), _pick(QR, c * BLOCKS + i)
        before = jnp.where(i == 0, 0, _field(_pick(TA, c * BLOCKS + _ready(c, i - 1) - 1), 2))
        before = jnp.where(jnp.logical_and(i > 0, _ready(c, i - 1) == _ready(c, i - 2)), _field(_pick(QA, c * BLOCKS + i - 1), 3), before)
        add(_field(qr, 0), _field(qr, 1))
        lax.fori_loop(before, _field(qa, 0), slot, None)

        @pl.when(b // 2 != c)
        def _():
            for j in range(UNITS):
                u = unit(b, 1 - k, j)
                remote(u, u, send_s.at[b * UNITS + j], recv_s.at[b * UNITS + j], sib).wait_recv()

        @pl.when(b == other)
        def _():
            for j in range(UNITS):
                u = unit(b, 1 - k, j)
                remote(u, u, send_o.at[j], recv_o.at[(1 - k) * UNITS + j], sib).wait_recv()

        tokens = pltpu.make_async_copy(xg.at[pl.ds(b * 8, 8)], xv, lsem.at[0])
        tokens.start()
        cos, sin = base_v[0, pl.ds(rows + b, 1), :], base_v[1, pl.ds(rows + b, 1), :]
        turn_v[0] = cos * base_v[0, :rows, :] - sin * base_v[1, :rows, :]
        turn_v[1] = sin * base_v[0, :rows, :] + cos * base_v[1, :rows, :]
        acc[...] = jnp.zeros(acc.shape, jnp.float32)
        tokens.wait()

        def project(s, _):
            g = i * steps + s

            @pl.when(g + 2 < BLOCKS * steps)
            def _():
                for cp in fetch_w(g + 2):
                    cp.start()

            for cp in fetch_w(g):
                cp.wait()
            a = xv[:, :, pl.ds(pl.multiple_of(s * depth, 128), depth)].reshape(rows, depth)
            for m in range(3):
                acc[m] = acc[m] + jnp.dot(a, wbuf[g % 3, m], preferred_element_type=jnp.float32)

            @pl.when(jnp.logical_or(s == 4, jnp.logical_or(s == 9, s == 13)))
            def _():
                n = s // 5
                lax.fori_loop(_field(qa, n), _field(qa, n + 1), slot, None)
                add(_field(qr, n + 1), _field(qr, n + 2))

        lax.fori_loop(0, steps, project, None)
        at = pl.ds(pl.multiple_of(b * rows, rows), rows)
        cos, sin = turn_v[0], turn_v[1]
        for h in range(heads):
            cols = slice(h * HEAD, (h + 1) * HEAD)
            q = acc[0, :, cols].astype(jnp.bfloat16).astype(jnp.float32)
            qv[place, h] = (q * cos + pltpu.roll(q, HEAD // 2, 1) * sin).astype(jnp.bfloat16)
            key = acc[1, :, cols].astype(jnp.bfloat16).astype(jnp.float32)
            kc[h, at, :] = (key * cos + pltpu.roll(key, HEAD // 2, 1) * sin).astype(jnp.bfloat16)
            vt[h, :HEAD, at] = acc[2, :, cols].T.astype(jnp.bfloat16)
        lax.fori_loop(jnp.where(i == 0, 0, _ready(c, i - 1)), _ready(c, i), finish, None)

    def finish(b, _):
        ta, tr = _pick(TA, c * BLOCKS + b), _pick(TR, c * BLOCKS + b)
        for j in range(2):
            fetch_wo(j).start()
        attend(b, jnp.where(b // 2 == c, b % 2, 2))
        lax.fori_loop(_field(ta, 0), _field(ta, 1), slot, None)
        add(_field(tr, 0), _field(tr, 1))

        def term(j, _):
            place = j % 2
            mine_out = pltpu.make_async_copy(tbuf.at[place, k], own_s.at[b, j], tsem.at[place])
            theirs_out = remote(tst.at[place], sib_in.at[b, j], tssem.at[place], recv_t.at[b * UNITS + j], sib)

            @pl.when(j >= 2)
            def _():
                mine_out.wait()
                theirs_out.wait_send()

            fetch_wo(j).wait()
            tbuf[place] = jnp.dot(ov[...], wobuf[place], preferred_element_type=jnp.float32).reshape(tbuf.shape[1:])

            @pl.when(j + 2 < UNITS)
            def _():
                fetch_wo(j + 2).start()

            tst[place] = tbuf[place, 1 - k].astype(jnp.bfloat16)
            mine_out.start()
            theirs_out.start()

        lax.fori_loop(0, UNITS, term, None)
        for place in range(2):
            pltpu.make_async_copy(tbuf.at[place, k], own_s.at[b, place], tsem.at[place]).wait()
            remote(tst.at[place], sib_in.at[b, place], tssem.at[place], recv_t.at[b * UNITS + place], sib).wait_send()
        lax.fori_loop(_field(ta, 1), _field(ta, 2), slot, None)
        add(_field(tr, 1), _field(tr, 2))

    lax.fori_loop(0, BLOCKS, work, None)
    add(_field(_pick(TR, c * BLOCKS + BLOCKS - 1), 2), BLOCKS * UNITS)

    for j in range(UNITS):
        remote(rs_own.at[0], sums.at[1 - k, :, pl.ds(j * wide, wide)], fsem.at[1], recv_f.at[j], sib).wait_recv()
    for n in range(8):
        own_to_sib(n // 4, n % 4).wait_send()

    def passed(i, _):
        b, j = i // UNITS, i % UNITS

        @pl.when(jnp.logical_and(jnp.logical_not(final), b <= 2 * c + 1))
        def _():
            to_right(b, j).wait_send()

        @pl.when(jnp.logical_and(jnp.logical_not(first), b >= 2 * c))
        def _():
            to_left(b, j).wait_send()

        @pl.when(b // 2 != c)
        def _():
            to_sib(b, j).wait_send()
            for q in range(2):
                low = land.at[b, j, pl.ds(q * (rs_own.shape[1] // 2), rs_own.shape[1] // 2)]
                remote(low, low, out_sem.at[i * 2 + q], recv_rr.at[i * 2 + q], left).wait_send()

    lax.fori_loop(0, BLOCKS * UNITS, passed, None)


def turns(rows):
    lane, at = jnp.arange(HEAD), jnp.arange(rows + BLOCKS)
    place = jnp.where(at < rows, at, (at - rows) * rows)
    half = HEAD // 2
    angle = place.astype(jnp.float32)[:, None] * THETA ** (-(lane % half).astype(jnp.float32) / half)
    return jnp.stack([jnp.cos(angle), jnp.where(lane < half, -1.0, 1.0) * jnp.sin(angle)])


def solution(mesh):
    def step(x, gain, wq, wk, wv, wo):
        rows, dim = x.shape
        width = wq.shape[1]
        heads, half, wide, depth = width // HEAD, rows // 2, dim // UNITS, dim // 14
        bf, f32 = jnp.bfloat16, jnp.float32
        hbm = pl.BlockSpec(memory_space=pl.ANY)
        dma = pltpu.SemaphoreType.DMA
        turn = turns(rows)
        shape = jax.ShapeDtypeStruct
        total, *_ = pl.pallas_call(
            layer,
            out_shape=[
                shape((2, half, dim), f32),
                shape((BLOCKS * 8, rows // 8, dim), bf),
                shape((BLOCKS, UNITS, half, wide), f32),
                shape((BLOCKS, UNITS, half, wide), bf),
            ],
            in_specs=[hbm] * 7,
            out_specs=[hbm] * 4,
            scratch_shapes=[
                pltpu.VMEM((8, rows // 8, dim), bf),
                pltpu.VMEM((dim // HEAD, HEAD), bf),
                pltpu.VMEM((2, rows, HEAD), f32),
                pltpu.VMEM((3, 3, depth, width), bf),
                pltpu.VMEM((2, width, wide), bf),
                pltpu.VMEM((3, rows, width), f32),
                pltpu.VMEM((3, heads, rows, HEAD), bf),
                pltpu.VMEM((heads, BLOCKS * rows, HEAD), bf),
                pltpu.VMEM((heads, HEAD + 16, BLOCKS * rows), bf),
                pltpu.VMEM((rows, width), bf),
                pltpu.VMEM((heads, rows), f32),
                pltpu.VMEM((heads, HEAD + 16, rows), f32),
                pltpu.VMEM((2, 2, half, wide), f32),
                pltpu.VMEM((2, half, wide), bf),
                pltpu.VMEM((2, half, wide), f32),
                pltpu.VMEM((2, half, wide), bf),
                pltpu.VMEM((BLOCKS + 2, UNITS, half, wide), bf),
                pltpu.VMEM((2, rows + BLOCKS, HEAD), f32),
                pltpu.VMEM((1, dim), f32),
                dma((8,)), dma((8,)), dma((2,)), dma((3, 3)), dma((2,)), dma((2,)), dma((2,)),
                dma((24,)), dma((32,)), dma((8,)), dma((32,)),
                dma((32,)), dma((32,)), dma((8,)), dma((32,)),
                dma((32,)), dma((64,)), dma((64,)), dma((4,)), dma((64,)), dma((2, 2)), dma((2,)),
            ],
            compiler_params=pltpu.CompilerParams(collective_id=0, has_side_effects=True, vmem_limit_bytes=67_043_328),
        )(x.reshape(8, rows // 8, dim), gain.reshape(dim // HEAD, HEAD), turn, wq, wk, wv, wo)
        return (x.astype(f32) + total.reshape(rows, dim)).astype(bf)

    tokens, columns = P(("dp", "tp"), None), P(None, "tp")
    return jax.shard_map(
        step,
        mesh=mesh,
        in_specs=(tokens, P(None), columns, columns, columns, P("tp", None)),
        out_specs=tokens,
        check_vma=False,
    )
```

```python
import functools

import jax
import jax.numpy as jnp
from jax import lax
from jax.experimental import pallas as pl
from jax.experimental.pallas import tpu as pltpu
from jax.sharding import PartitionSpec as P

HEAD = 128
THETA = 10000
NEG = -1e30
HIDDEN = 2 * NEG
LOG2E = 1.4426950408889634
CHIPS = 4
BLOCKS = 8
UNITS = 4
MESH = pl.DeviceIdType.MESH


def _dot(a, b, ca, cb):
    return lax.dot_general(a, b, (((ca,), (cb,)), ((), ())), preferred_element_type=jnp.float32)


QA = [266240, 1061058, 1597764, 2396680, 3461900, 4527120, 5592340, 6391320, 266240, 794753, 1331460, 2396680, 3724108, 4260815, 4260880, 4260880, 0, 266240, 1331460, 2662984, 3724108, 4260880, 4260880, 4260880, 0, 0, 1331460, 2396680, 3461900, 5059728, 6120852, 6391320]
QR = [0, 0, 0, 68174084, 102261126, 170435210, 238609294, 306783378, 0, 0, 0, 0, 0, 50593792, 203981190, 306516943, 0, 0, 0, 16777216, 68169858, 136077637, 238342859, 323560464, 0, 0, 0, 68174084, 136348168, 204522252, 272696336, 340870420]
TA = [8257, 16644, 29126, 41609, 58253, 74897, 91541, 99864, 24965, 41609, 45706, 49867, 62350, 66576, 66576, 66576, 24965, 45770, 62350, 66576, 66576, 66576, 66576, 66576, 24901, 41609, 58253, 83219, 99799, 99864, 99864, 99864]
TR = [0, 0, 16384, 24836, 41350, 57994, 74638, 91282, 0, 0, 0, 0, 0, 24835, 62284, 79058, 0, 8257, 20740, 37384, 41609, 45770, 66446, 83219, 16384, 33028, 49672, 66316, 82960, 99604, 99864, 99864]
ORDER = [449161512, 726256176, 934077174, 34601916, 183963746, 230, 86033424, 189944419, 864279766, 365208442, 1072083883, 494, 172066848, 379887846, 855390636, 991458170, 1062894194, 758, 172066848, 379887846, 587708844, 795529842, 1003350840, 1022]


def _pick(table, at):
    got = 0
    for i, v in enumerate(table):
        got = got + jnp.where(at == i, v, 0)
    return got


def _field(word, n, bits=6):
    return lax.shift_right_logical(word, bits * n) & (2**bits - 1)


def _block(c, i):
    j = i - 2
    return jnp.where(c == 0, i, jnp.where(i < 2, 2 * c + i, jnp.where(j < 2 * c, j, i)))


def _ready(c, i):
    rest = jnp.where(i < 2, 0, jnp.where(i - 1 < 2 * c, i - 1, i + 1))
    return jnp.where(c == 0, i + 1, rest)


def layer(x_ref, gain_ref, turn_ref, wq_ref, wk_ref, wv_ref, wo_ref, sums, xg, own_s, sib_in,
          xv, gain_v, turn_v, wbuf, wobuf, acc, qv, kc, vt, ov, top_s, mix_s, tbuf, tst, rs_own, rs_sib, land,
          base_v, row_v, xsem, ksem, lsem, wsem, osem, tsem, tssem, recv_r, recv_l, recv_o, recv_s, send_r, send_l, send_o, send_s,
          recv_t, recv_rl, recv_rr, recv_f, out_sem, rsem, fsem):
    t = lax.axis_index("tp")
    c, k = t // 2, t % 2
    me, sib, left, right = {"tp": t}, {"tp": t + 1 - 2 * k}, {"tp": t - 2}, {"tp": t + 2}
    mine, other = 2 * c + k, 2 * c + 1 - k
    heads, rows = qv.shape[1], qv.shape[2]
    depth, width = wbuf.shape[2], wbuf.shape[3]
    steps = xv.shape[2] // depth
    wide = wobuf.shape[2]
    first, final = c == 0, c == CHIPS - 1

    def remote(src, dst, ssem, rsem, to):
        return pltpu.make_async_remote_copy(src_ref=src, dst_ref=dst, send_sem=ssem, recv_sem=rsem, device_id=to, device_id_type=MESH)

    def unit(b, h, j):
        return xg.at[(b * 2 + h) * UNITS + j]

    def to_right(b, j):
        u = unit(b, k, j)
        return remote(u, u, send_r.at[b * UNITS + j], recv_r.at[b * UNITS + j], right)

    def to_left(b, j):
        u = unit(b, k, j)
        return remote(u, u, send_l.at[b * UNITS + j], recv_l.at[b * UNITS + j], left)

    def to_sib(b, j):
        u = unit(b, k, j)
        return remote(u, u, send_s.at[b * UNITS + j], recv_s.at[b * UNITS + j], sib)

    def own_to_sib(h, j):
        u = unit(mine, h, j)
        return remote(u, u, send_o.at[h * UNITS + j], recv_o.at[h * UNITS + j], sib)

    def fetch_w(g):
        at, slot = pl.multiple_of((g % steps) * depth, depth), g % 3
        return [pltpu.make_async_copy(w.at[pl.ds(at, depth), :], wbuf.at[slot, i], wsem.at[slot, i])
                for i, w in enumerate((wq_ref, wk_ref, wv_ref))]

    def fetch_wo(j):
        return pltpu.make_async_copy(wo_ref.at[:, pl.ds(pl.multiple_of(j * wide, 128), wide)], wobuf.at[j % 2], osem.at[j % 2])

    barrier = pltpu.get_barrier_semaphore()
    pl.semaphore_signal(barrier, inc=1, device_id=sib, device_id_type=MESH)

    @pl.when(jnp.logical_not(first))
    def _():
        pl.semaphore_signal(barrier, inc=1, device_id=left, device_id_type=MESH)

    @pl.when(jnp.logical_not(final))
    def _():
        pl.semaphore_signal(barrier, inc=1, device_id=right, device_id_type=MESH)

    def half_of(n):
        return jnp.where(n % 2 == 0, 1 - k, k)

    def load_x(n):
        u = half_of(n) * UNITS + n // 2
        return pltpu.make_async_copy(x_ref.at[u], xv.at[u], xsem.at[n])

    def keep_x(n):
        u = half_of(n) * UNITS + n // 2
        return pltpu.make_async_copy(xv.at[u], xg.at[mine * 8 + u], ksem.at[n])

    load_g = pltpu.make_async_copy(gain_ref, gain_v, lsem.at[0])
    load_t = pltpu.make_async_copy(turn_ref, base_v, lsem.at[1])
    load_g.start()
    for n in range(8):
        load_x(n).start()
    load_t.start()
    for g in range(2):
        for cp in fetch_w(g):
            cp.start()
    load_g.wait()
    for n in range(gain_v.shape[0]):
        row_v[:, n * HEAD : (n + 1) * HEAD] = gain_v[n : n + 1, :].astype(jnp.float32)

    middle = jnp.logical_and(jnp.logical_not(first), jnp.logical_not(final))

    @pl.when(middle)
    def _():
        pl.semaphore_wait(barrier, 3)

    @pl.when(jnp.logical_not(middle))
    def _():
        pl.semaphore_wait(barrier, 2)

    def link(b, j, i):
        @pl.when(jnp.logical_not(first))
        def _():
            to_left(b, j).start()

        @pl.when(jnp.logical_or(first, jnp.logical_and(jnp.logical_not(final), i < 1 * c)))
        def _():
            to_right(b, j).start()

    def norm(n, _):
        @pl.when(n < 8)
        def _():
            u, some = half_of(n) * UNITS + n // 2, xv.shape[1] // 2
            load_x(n).wait()
            for m in range(2):
                here = slice(m * some, (m + 1) * some)
                wx = xv[u, here, :].astype(jnp.float32)
                scale = lax.rsqrt(jnp.mean(wx * wx, -1, keepdims=True) + 1e-6)
                xv[u, here, :] = (wx * scale * row_v[...]).astype(jnp.bfloat16)
            keep_x(n).start()

        @pl.when(n > 0)
        def _():
            h, j = half_of(n - 1), (n - 1) // 2
            keep_x(n - 1).wait()
            own_to_sib(h, j).start()

            @pl.when(jnp.logical_and(h == k, k == 0))
            def _():
                link(mine, j, j)

    lax.fori_loop(0, 9, norm, None)

    def begin(i, _):
        b, j = 2 * c + i // UNITS, i % UNITS

        @pl.when(b == other)
        def _():
            u = unit(other, k, j)
            remote(u, u, send_o.at[k * UNITS + j], recv_o.at[k * UNITS + j], sib).wait_recv()

        link(b, j, i)

    lax.fori_loop(UNITS * (1 - k), 2 * UNITS, begin, None)
    load_t.wait()
    for h in range(heads):
        vt[h, HEAD:, :] = jnp.ones((vt.shape[1] - HEAD, vt.shape[2]), jnp.bfloat16)

    def slot(i, _):
        j = i % UNITS

        @pl.when(i < 8 * c)
        def _():
            b = i // UNITS
            to_right(b, j).wait_recv()

            @pl.when(jnp.logical_not(final))
            def _():
                to_right(b, j).start()

            to_sib(b, j).start()

            @pl.when(jnp.logical_and(jnp.logical_not(final), i == 8 * c - 1))
            def _():
                def own(n, _):
                    to_right(2 * c + n // UNITS, n % UNITS).start()

                lax.fori_loop(1 * c, 2 * UNITS, own, None)

        @pl.when(i < 8 * (CHIPS - 1 - c))
        def _():
            b = 2 * c + 2 + i // UNITS
            to_left(b, j).wait_recv()

            @pl.when(jnp.logical_not(first))
            def _():
                to_left(b, j).start()

            to_sib(b, j).start()

    def attend(b, place):
        e = HEAD**-0.5 * LOG2E
        top_s[...] = jnp.full(top_s.shape, NEG, jnp.float32)
        mix_s[...] = jnp.zeros(mix_s.shape, jnp.float32)

        def block(j, masked):
            here = pl.ds(pl.multiple_of(j * rows, rows), rows)
            scores = [_dot(kc[h, here, :], qv[place, h], 1, 1) for h in range(heads)]
            weights, keeps = [], []
            for h, s in enumerate(scores):
                if masked:
                    ok = lax.broadcasted_iota(jnp.int32, s.shape, 1) >= lax.broadcasted_iota(jnp.int32, s.shape, 0)
                    s = jnp.where(ok, s, HIDDEN)
                old = top_s[h : h + 1, :]
                top = jnp.maximum(old, s.max(axis=0, keepdims=True))
                top_s[h : h + 1, :] = top
                weights.append(jnp.exp2((s - top) * e).astype(jnp.bfloat16))
                keeps.append(jnp.exp2((old - top) * e))
            for h in range(heads):
                mix_s[h] = mix_s[h] * keeps[h] + _dot(vt[h, :, here], weights[h], 1, 0)

        lax.fori_loop(0, b, lambda j, _: block(j, False), None)
        block(b, True)
        for h in range(heads):
            total = mix_s[h, HEAD : HEAD + 1, :]
            ov[:, h * HEAD : (h + 1) * HEAD] = (mix_s[h, :HEAD, :] * (1 / total)).T.astype(jnp.bfloat16)

    def nth(r):
        u = _field(_pick(ORDER, c * 6 + r // 6), r % 6, 5)
        return u // UNITS, u % UNITS

    def loads(r, b, j):
        return [pltpu.make_async_copy(own_s.at[b, j], rs_own.at[r % 2], rsem.at[r % 2, 0]),
                pltpu.make_async_copy(sib_in.at[b, j], rs_sib.at[r % 2], rsem.at[r % 2, 1])]

    def ask(r):
        b, j = nth(r)
        remote(tst.at[0], sib_in.at[b, j], tssem.at[0], recv_t.at[b * UNITS + j], sib).wait_recv()
        for cp in loads(r, b, j):
            cp.start()

    def add(start, end):
        @pl.when(start < end)
        def _():
            ask(start)

        def one(r, _):
            @pl.when(r + 1 < end)
            def _():
                ask(r + 1)

            b, j = nth(r)
            d, p = b // 2, r % 2
            for cp in loads(r, b, j):
                cp.wait()
            for q in range(2):
                some = pl.ds(q * (rs_own.shape[1] // 2), rs_own.shape[1] // 2)
                at = (b * UNITS + j) * 2 + q
                high, low = land.at[b + 2, j, some], land.at[b, j, some]
                rs_own[p, some] = rs_own[p, some] + rs_sib[p, some].astype(jnp.float32)

                @pl.when(jnp.logical_and(d >= c, jnp.logical_not(first)))
                def _():
                    remote(high, high, out_sem.at[at], recv_rl.at[at], left).wait_recv()
                    rs_own[p, some] = rs_own[p, some] + high[...].astype(jnp.float32)

                @pl.when(jnp.logical_and(d <= c, jnp.logical_not(final)))
                def _():
                    remote(low, low, out_sem.at[at], recv_rr.at[at], right).wait_recv()
                    rs_own[p, some] = rs_own[p, some] + low[...].astype(jnp.float32)

                @pl.when(d > c)
                def _():
                    high[...] = rs_own[p, some].astype(jnp.bfloat16)
                    remote(high, high, out_sem.at[at], recv_rl.at[at], right).start()

                @pl.when(d < c)
                def _():
                    low[...] = rs_own[p, some].astype(jnp.bfloat16)
                    remote(low, low, out_sem.at[at], recv_rr.at[at], left).start()

            result = sums.at[k, :, pl.ds(pl.multiple_of(j * wide, 128), wide)]

            @pl.when(b == mine)
            def _():
                cp = pltpu.make_async_copy(rs_own.at[p], result, fsem.at[0])
                cp.start()
                cp.wait()

            @pl.when(b == other)
            def _():
                cp = remote(rs_own.at[p], result, fsem.at[1], recv_f.at[j], sib)
                cp.start()
                cp.wait_send()

        lax.fori_loop(start, end, one, None)

    def work(i, _):
        b = _block(c, i)
        place = jnp.where(b // 2 == c, b % 2, 2)
        qa, qr = _pick(QA, c * BLOCKS + i), _pick(QR, c * BLOCKS + i)
        before = jnp.where(i == 0, 0, _field(_pick(TA, c * BLOCKS + _ready(c, i - 1) - 1), 2))
        before = jnp.where(jnp.logical_and(i > 0, _ready(c, i - 1) == _ready(c, i - 2)), _field(_pick(QA, c * BLOCKS + i - 1), 3), before)
        add(_field(qr, 0), _field(qr, 1))
        lax.fori_loop(before, _field(qa, 0), slot, None)

        @pl.when(b // 2 != c)
        def _():
            for j in range(UNITS):
                u = unit(b, 1 - k, j)
                remote(u, u, send_s.at[b * UNITS + j], recv_s.at[b * UNITS + j], sib).wait_recv()

        @pl.when(b == other)
        def _():
            for j in range(UNITS):
                u = unit(b, 1 - k, j)
                remote(u, u, send_o.at[j], recv_o.at[(1 - k) * UNITS + j], sib).wait_recv()

        tokens = pltpu.make_async_copy(xg.at[pl.ds(b * 8, 8)], xv, lsem.at[0])
        tokens.start()
        cos, sin = base_v[0, pl.ds(rows + b, 1), :], base_v[1, pl.ds(rows + b, 1), :]
        turn_v[0] = cos * base_v[0, :rows, :] - sin * base_v[1, :rows, :]
        turn_v[1] = sin * base_v[0, :rows, :] + cos * base_v[1, :rows, :]
        acc[...] = jnp.zeros(acc.shape, jnp.float32)
        tokens.wait()

        def project(s, _):
            g = i * steps + s

            @pl.when(g + 2 < BLOCKS * steps)
            def _():
                for cp in fetch_w(g + 2):
                    cp.start()

            for cp in fetch_w(g):
                cp.wait()
            a = xv[:, :, pl.ds(pl.multiple_of(s * depth, 128), depth)].reshape(rows, depth)
            for m in range(3):
                acc[m] = acc[m] + jnp.dot(a, wbuf[g % 3, m], preferred_element_type=jnp.float32)

            @pl.when(jnp.logical_or(s == 4, jnp.logical_or(s == 9, s == 13)))
            def _():
                n = s // 5
                lax.fori_loop(_field(qa, n), _field(qa, n + 1), slot, None)
                add(_field(qr, n + 1), _field(qr, n + 2))

        lax.fori_loop(0, steps, project, None)
        at = pl.ds(pl.multiple_of(b * rows, rows), rows)
        cos, sin = turn_v[0], turn_v[1]
        for h in range(heads):
            cols = slice(h * HEAD, (h + 1) * HEAD)
            q = acc[0, :, cols].astype(jnp.bfloat16).astype(jnp.float32)
            qv[place, h] = (q * cos + pltpu.roll(q, HEAD // 2, 1) * sin).astype(jnp.bfloat16)
            key = acc[1, :, cols].astype(jnp.bfloat16).astype(jnp.float32)
            kc[h, at, :] = (key * cos + pltpu.roll(key, HEAD // 2, 1) * sin).astype(jnp.bfloat16)
            vt[h, :HEAD, at] = acc[2, :, cols].T.astype(jnp.bfloat16)
        lax.fori_loop(jnp.where(i == 0, 0, _ready(c, i - 1)), _ready(c, i), finish, None)

    def finish(b, _):
        ta, tr = _pick(TA, c * BLOCKS + b), _pick(TR, c * BLOCKS + b)
        for j in range(2):
            fetch_wo(j).start()
        attend(b, jnp.where(b // 2 == c, b % 2, 2))
        lax.fori_loop(_field(ta, 0), _field(ta, 1), slot, None)
        add(_field(tr, 0), _field(tr, 1))

        def term(j, _):
            place = j % 2
            mine_out = pltpu.make_async_copy(tbuf.at[place, k], own_s.at[b, j], tsem.at[place])
            theirs_out = remote(tst.at[place], sib_in.at[b, j], tssem.at[place], recv_t.at[b * UNITS + j], sib)

            @pl.when(j >= 2)
            def _():
                mine_out.wait()
                theirs_out.wait_send()

            fetch_wo(j).wait()
            tbuf[place] = jnp.dot(ov[...], wobuf[place], preferred_element_type=jnp.float32).reshape(tbuf.shape[1:])

            @pl.when(j + 2 < UNITS)
            def _():
                fetch_wo(j + 2).start()

            tst[place] = tbuf[place, 1 - k].astype(jnp.bfloat16)
            mine_out.start()
            theirs_out.start()

        lax.fori_loop(0, UNITS, term, None)
        for place in range(2):
            pltpu.make_async_copy(tbuf.at[place, k], own_s.at[b, place], tsem.at[place]).wait()
            remote(tst.at[place], sib_in.at[b, place], tssem.at[place], recv_t.at[b * UNITS + place], sib).wait_send()
        lax.fori_loop(_field(ta, 1), _field(ta, 2), slot, None)
        add(_field(tr, 1), _field(tr, 2))

    lax.fori_loop(0, BLOCKS, work, None)
    add(_field(_pick(TR, c * BLOCKS + BLOCKS - 1), 2), BLOCKS * UNITS)

    for j in range(UNITS):
        remote(rs_own.at[0], sums.at[1 - k, :, pl.ds(j * wide, wide)], fsem.at[1], recv_f.at[j], sib).wait_recv()
    for n in range(8):
        own_to_sib(n // 4, n % 4).wait_send()

    def passed(i, _):
        b, j = i // UNITS, i % UNITS

        @pl.when(jnp.logical_and(jnp.logical_not(final), b <= 2 * c + 1))
        def _():
            to_right(b, j).wait_send()

        @pl.when(jnp.logical_and(jnp.logical_not(first), b >= 2 * c))
        def _():
            to_left(b, j).wait_send()

        @pl.when(b // 2 != c)
        def _():
            to_sib(b, j).wait_send()
            for q in range(2):
                low = land.at[b, j, pl.ds(q * (rs_own.shape[1] // 2), rs_own.shape[1] // 2)]
                remote(low, low, out_sem.at[i * 2 + q], recv_rr.at[i * 2 + q], left).wait_send()

    lax.fori_loop(0, BLOCKS * UNITS, passed, None)


def turns(rows):
    lane, at = jnp.arange(HEAD), jnp.arange(rows + BLOCKS)
    place = jnp.where(at < rows, at, (at - rows) * rows)
    half = HEAD // 2
    angle = place.astype(jnp.float32)[:, None] * THETA ** (-(lane % half).astype(jnp.float32) / half)
    return jnp.stack([jnp.cos(angle), jnp.where(lane < half, -1.0, 1.0) * jnp.sin(angle)])


def solution(mesh):
    def step(x, gain, wq, wk, wv, wo):
        rows, dim = x.shape
        width = wq.shape[1]
        heads, half, wide, depth = width // HEAD, rows // 2, dim // UNITS, dim // 14
        bf, f32 = jnp.bfloat16, jnp.float32
        hbm = pl.BlockSpec(memory_space=pl.ANY)
        dma = pltpu.SemaphoreType.DMA
        turn = turns(rows)
        shape = jax.ShapeDtypeStruct
        total, *_ = pl.pallas_call(
            layer,
            out_shape=[
                shape((2, half, dim), f32),
                shape((BLOCKS * 8, rows // 8, dim), bf),
                shape((BLOCKS, UNITS, half, wide), f32),
                shape((BLOCKS, UNITS, half, wide), bf),
            ],
            in_specs=[hbm] * 7,
            out_specs=[hbm] * 4,
            scratch_shapes=[
                pltpu.VMEM((8, rows // 8, dim), bf),
                pltpu.VMEM((dim // HEAD, HEAD), bf),
                pltpu.VMEM((2, rows, HEAD), f32),
                pltpu.VMEM((3, 3, depth, width), bf),
                pltpu.VMEM((2, width, wide), bf),
                pltpu.VMEM((3, rows, width), f32),
                pltpu.VMEM((3, heads, rows, HEAD), bf),
                pltpu.VMEM((heads, BLOCKS * rows, HEAD), bf),
                pltpu.VMEM((heads, HEAD + 16, BLOCKS * rows), bf),
                pltpu.VMEM((rows, width), bf),
                pltpu.VMEM((heads, rows), f32),
                pltpu.VMEM((heads, HEAD + 16, rows), f32),
                pltpu.VMEM((2, 2, half, wide), f32),
                pltpu.VMEM((2, half, wide), bf),
                pltpu.VMEM((2, half, wide), f32),
                pltpu.VMEM((2, half, wide), bf),
                pltpu.VMEM((BLOCKS + 2, UNITS, half, wide), bf),
                pltpu.VMEM((2, rows + BLOCKS, HEAD), f32),
                pltpu.VMEM((1, dim), f32),
                dma((8,)), dma((8,)), dma((2,)), dma((3, 3)), dma((2,)), dma((2,)), dma((2,)),
                dma((24,)), dma((32,)), dma((8,)), dma((32,)),
                dma((32,)), dma((32,)), dma((8,)), dma((32,)),
                dma((32,)), dma((64,)), dma((64,)), dma((4,)), dma((64,)), dma((2, 2)), dma((2,)),
            ],
            compiler_params=pltpu.CompilerParams(collective_id=0, has_side_effects=True, vmem_limit_bytes=67_043_328),
        )(x.reshape(8, rows // 8, dim), gain.reshape(dim // HEAD, HEAD), turn, wq, wk, wv, wo)
        return (x.astype(f32) + total.reshape(rows, dim)).astype(bf)

    tokens, columns = P(("dp", "tp"), None), P(None, "tp")
    return jax.shard_map(
        step,
        mesh=mesh,
        in_specs=(tokens, P(None), columns, columns, columns, P("tp", None)),
        out_specs=tokens,
        check_vma=False,
    )
```
